512 devices in a mesh: slab: 128 (over x, z, y_hi), blk: 4 (over y_lo, core).
Axes of the slice: x: 4, y: 8 (y_hi: 4, y_lo: 2; y = y_hi * 2 + y_lo), z: 8, core: 2. Of those that a mesh axis runs over, the one named last changes fastest.
Arguments:
- incident: float32 [256, 2, 336, 128], P('slab', None, 'blk'), may hold values from -6 to 6
- mie_coef: float32 [256, 2, 336], P('slab', None, 'blk'), may hold values from -0.6 to 0.6
- translation: bfloat16 [256, 8, 2, 336, 336], P('slab', None, None, 'blk'), may hold values from -0.078125 to 0.078125
- pair_shift: int32 [256, 8], P('slab'), may hold values from -1 to 1
- pair_member: int32 [256, 8], P('slab'), may hold values from 0 to 1
- positions: float32 [256, 3], P('slab'), may hold values from 0 to 1
- wave_index: int32 [256, 3], replicated, may hold values from -4 to 4
- plane_coef: bfloat16 [256, 2, 336], replicated, may hold values from -0.25 to 0.25
- ewald_weight: float32 [256], replicated, may hold values from 0.002 to 0.04
Outputs:
- basis_next: float32 [256, 2, 336, 128], P('slab', None, 'blk')
- residual: float32 [256, 2, 336, 128], P('slab', None, 'blk')
- hessenberg: float32 [9, 128], replicated
The draws below stay inside these ranges and needn't reach their ends.
Inputs may be any that keep to these rules, and one draw needn't show every extreme that they name: `pair_shift`: each pair's source sphere lies in the target's slab or in one of the two slabs beside it on the periodic cycle of slabs.
All inputs are finite; a program needn't handle non-finite values.
Results may differ from the reference program's by a relative error of at most 0.004.
Values may be sent and summed in bfloat16 or wider, within the bound.
A program may use at most 64 MiB of HBM per device.

```python
import math
import jax
import jax.numpy as jnp
from jax import lax

COEF = 336
K = 8
NG = 256
SPH_DEV = 2
RHS = 128
SPHERES = 256
N_SLAB = 128


def draw_mie_coef(key, part):
    sub_one = jax.random.fold_in(key, 71)
    place = jnp.arange(SPHERES, dtype=jnp.float32) / max(SPHERES - 1, 1)
    values = jax.random.uniform(sub_one, (SPHERES, 2, COEF), jnp.float32, -0.6, 0.6)
    ramp = 0.3 + 0.7 * place
    return (values * ramp[:, None, None]).astype(jnp.float32)


def set_ends(array, rng, least, largest):
    dims = array.shape
    index_at = [jax.random.randint(jax.random.fold_in(rng, axis), (), 0, dims[axis]) for axis in range(len(dims))]
    array = array.at[tuple(index_at)].set(least)
    longest = dims.index(max(dims))
    index_at[longest] = (index_at[longest] + 1) % dims[longest]
    return array.at[tuple(index_at)].set(largest)


def block_scale(stream_key, extent, pieces, least, top_value):
    def one(position, shards_of):
        draws = jax.random.uniform(jax.random.fold_in(jax.random.fold_in(stream_key, 6), position), (shards_of,), jnp.float32, least / len(pieces), top_value / len(pieces))
        return jnp.repeat(jnp.exp(draws), extent[position] // shards_of).reshape((-1,) + (1,) * (len(extent) - position - 1))

    loudness = one(*pieces[0])
    for cut in pieces[1:]:
        loudness = loudness * one(*cut)
    return loudness


def gaussian(key, shape, scale, limit, shards=(), held_as=jnp.bfloat16):
    factor_of = block_scale(key, shape, shards, -0.22, 0.18) if shards else 1.0
    array = jax.random.normal(key, shape, jnp.float32) * scale * factor_of
    return jnp.minimum(jnp.maximum(array, -limit), limit).astype(held_as)


def setup_inputs(seed: int = 0) -> dict:
    arg_keys = jax.random.split(jax.random.key(seed), 10)
    incident = gaussian(arg_keys[0], (SPHERES, 2, COEF, RHS), 1.0, 6.0, ((0, 128), (2, 4)), jnp.float32)
    mie_coef = draw_mie_coef(jax.random.fold_in(arg_keys[9], 71), 0)
    translation = gaussian(arg_keys[2], (SPHERES, K, 2, COEF, COEF), (2 * COEF * K) ** -0.5, 0.078125, ((0, 128), (3, 4)))
    pair_shift = set_ends(jax.random.randint(arg_keys[3], (SPHERES, K), -1, 2), jax.random.fold_in(arg_keys[3], 1), -1, 1).astype(jnp.int32)
    pair_member = set_ends(jax.random.randint(arg_keys[4], (SPHERES, K), 0, SPH_DEV), jax.random.fold_in(arg_keys[4], 1), 0, SPH_DEV - 1).astype(jnp.int32)
    positions = jnp.clip(1.0 * jax.random.uniform(arg_keys[5], (SPHERES, 3), jnp.float32) ** block_scale(arg_keys[5], (SPHERES, 3), ((0, 128),), -0.2, 0.2), 0.0, 1.0)
    wave_index = set_ends(jax.random.randint(arg_keys[6], (NG, 3), -4, 5), jax.random.fold_in(arg_keys[6], 1), -4, 4).astype(jnp.int32)
    plane_coef = gaussian(arg_keys[7], (NG, 2, COEF), (2 * COEF) ** -0.5, 0.25)
    ewald_weight = jnp.clip(jnp.exp(jax.random.uniform(arg_keys[8], (NG,), jnp.float32, math.log(0.002), math.log(0.04))), 0.002, 0.04)
    return {"incident": incident, "mie_coef": mie_coef, "translation": translation, "pair_shift": pair_shift, "pair_member": pair_member, "positions": positions, "wave_index": wave_index, "plane_coef": plane_coef, "ewald_weight": ewald_weight}


two_pi = 6.283185307179586
epsilon = 1e-06
highest = lax.Precision.HIGHEST

def complex_scale(coef_pair, basis):
    part_re = coef_pair[0] * basis[:, 0] - coef_pair[1] * basis[:, 1]
    part_im = coef_pair[0] * basis[:, 1] + coef_pair[1] * basis[:, 0]
    return jnp.stack([part_re, part_im], axis=1)

def inner_sum(left, right):
    part_re = lax.optimization_barrier(jnp.sum(left[:, 0] * right[:, 0] + left[:, 1] * right[:, 1], axis=(0, 1)))
    part_im = lax.optimization_barrier(jnp.sum(left[:, 0] * right[:, 1] - left[:, 1] * right[:, 0], axis=(0, 1)))
    return jnp.stack([part_re, part_im])

def plane_sums(projected, cos_part, sin_part):
    part_re = projected[:, 0, :, 0] - projected[:, 1, :, 1]
    part_im = projected[:, 0, :, 1] + projected[:, 1, :, 0]
    sum_re = lax.optimization_barrier(jnp.sum(cos_part[:, :, None] * part_re + sin_part[:, :, None] * part_im, axis=1))
    sum_im = lax.optimization_barrier(jnp.sum(cos_part[:, :, None] * part_im - sin_part[:, :, None] * part_re, axis=1))
    return jnp.stack([sum_re, sum_im], axis=1)

def plane_field(totals, coef_full, cos_part, sin_part, weights):
    total_re = totals[:, 0][:, None, :]
    total_im = totals[:, 1][:, None, :]
    turn_re = weights[:, None, None] * (cos_part[:, :, None] * total_re - sin_part[:, :, None] * total_im)
    turn_im = weights[:, None, None] * (cos_part[:, :, None] * total_im + sin_part[:, :, None] * total_re)
    turned = jnp.stack([turn_re, turn_im], axis=1)
    projected = jnp.einsum('gac,gbjn->jabcn', coef_full, turned, precision=highest)
    return jnp.stack([projected[:, 0, 0] + projected[:, 1, 1], projected[:, 0, 1] - projected[:, 1, 0]], axis=1)

def near_field(rounded, translation, pair_shift, pair_member):

    def per_slab(slab_index):
        start_row = slab_index * SPH_DEV
        matrices = lax.dynamic_slice_in_dim(translation, start_row, SPH_DEV, 0).astype(jnp.float32)
        offsets = lax.dynamic_slice_in_dim(pair_shift, start_row, SPH_DEV, 0)
        member = lax.dynamic_slice_in_dim(pair_member, start_row, SPH_DEV, 0)
        source = (jnp.mod(slab_index + offsets, N_SLAB) * SPH_DEV + member).reshape(-1).astype(jnp.int32)
        gathered = jnp.take(rounded, source, axis=0)
        product = jnp.einsum('parc,pzcn->pazrn', matrices.reshape(SPH_DEV * K, 2, COEF, COEF), gathered, precision=highest)
        near_re = product[:, 0, 0] - product[:, 1, 1]
        near_im = product[:, 0, 1] + product[:, 1, 0]
        return jnp.stack([near_re, near_im], axis=1).reshape(SPH_DEV, K, 2, COEF, RHS).sum(axis=1)
    blocks = lax.map(per_slab, jnp.arange(N_SLAB, dtype=jnp.int32))
    return blocks.reshape(SPH_DEV * N_SLAB, 2, COEF, RHS)

def apply_operator(vector, mie_coef, translation, pair_shift, pair_member, cos_part, sin_part, coef_full, ewald_weight):
    rounded = lax.optimization_barrier(vector.astype(jnp.bfloat16)).astype(jnp.float32)
    near = near_field(rounded, translation, pair_shift, pair_member)
    projected = jnp.einsum('gac,jbcn->gajbn', coef_full, rounded, precision=highest)
    totals = plane_sums(projected, cos_part, sin_part)
    far = plane_field(totals, coef_full, cos_part, sin_part, ewald_weight)
    summed = near + far
    scaled_re = mie_coef[:, 0][:, :, None] * summed[:, 0] - mie_coef[:, 1][:, :, None] * summed[:, 1]
    scaled_im = mie_coef[:, 0][:, :, None] * summed[:, 1] + mie_coef[:, 1][:, :, None] * summed[:, 0]
    return vector - jnp.stack([scaled_re, scaled_im], axis=1)

def reference(incident, mie_coef, translation, pair_shift, pair_member, positions, wave_index, plane_coef, ewald_weight):
    entries = SPHERES * COEF
    angles = two_pi * lax.optimization_barrier(jnp.sum(wave_index.astype(jnp.float32)[:, None, :] * positions[None, :, :], axis=-1))
    cos_part = jnp.cos(angles)
    sin_part = jnp.sin(angles)
    coef_full = plane_coef.astype(jnp.float32)

    def operator(vector):
        return apply_operator(vector, mie_coef, translation, pair_shift, pair_member, cos_part, sin_part, coef_full, ewald_weight)
    beta = jnp.sqrt(lax.optimization_barrier(jnp.sum(incident * incident, axis=(0, 1, 2))) / entries + epsilon)
    first = incident / beta
    image = operator(first)
    h_one_one = inner_sum(first, image) / entries
    image = image - complex_scale(h_one_one, first)
    h_two_one = jnp.sqrt(lax.optimization_barrier(jnp.sum(image * image, axis=(0, 1, 2))) / entries + epsilon)
    basis_next = image / h_two_one
    image = operator(basis_next)
    h_one_two = inner_sum(first, image) / entries
    image = image - complex_scale(h_one_two, first)
    h_two_two = inner_sum(basis_next, image) / entries
    residual = image - complex_scale(h_two_two, basis_next)
    h_three_two = jnp.sqrt(lax.optimization_barrier(jnp.sum(residual * residual, axis=(0, 1, 2))) / entries + epsilon)
    hessenberg = jnp.stack([beta, h_one_one[0], h_one_one[1], h_two_one, h_one_two[0], h_one_two[1], h_two_two[0], h_two_two[1], h_three_two])
    return (basis_next, residual, hessenberg)
```

```python
import functools

import jax
import jax.numpy as jnp
from jax import lax
from jax.experimental import pallas as pl
from jax.experimental.pallas import tpu as pltpu
from jax.sharding import PartitionSpec as P

MESH = pl.DeviceIdType.MESH
SLAB = "slab"
BLK = "blk"
two_pi = 6.283185307179586
epsilon = 1e-06

ROWS = 16


def pair_swap(field, even):
    count = field.shape[0]
    return jnp.where(even, pltpu.roll(field, count - 1, 0), pltpu.roll(field, 1, 0))


def complex_rows(coef_re, coef_im, field, swapped, even):
    return coef_re * field + jnp.where(even, -coef_im, coef_im) * swapped


def inner_rows(left, right, right_swapped, even):
    real = jnp.sum(left * right, axis=0, keepdims=True)
    cross = left * right_swapped
    imag = jnp.sum(jnp.where(even, cross, -cross), axis=0, keepdims=True)
    return real, imag


def kernel(
    quads,
    highs,
    spheres,
    pairs,
    coefs,
    entries,
    source_ref,
    start_ref,
    gather_ref,
    spread_ref,
    trig_ref,
    mie_ref,
    trans_ref,
    next_ref,
    residual_ref,
    hess_ref,
    piece_ref,
    halo_ref,
    stage_ref,
    join_ref,
    joined_ref,
    cut_ref,
    part_ref,
    line_ref,
    sums_ref,
    gram_ref,
    near_ref,
    send_sem,
    recv_sem,
    halo_sem,
):
    blocks = 4
    slabs = quads * highs
    line_size = highs * blocks
    slab = lax.axis_index(SLAB)
    blk = lax.axis_index(BLK)
    quad = slab // highs
    high = slab % highs
    core = blk % 2
    low = blk // 2
    spot = high * blocks + blk
    rows = coefs // blocks
    wide = 2 * rows
    total = spheres * wide
    waves = gather_ref.shape[0] // 2

    def plane_peer(step):
        return (lax.rem(quad + step, quads) * highs + high, blk)

    def line_peer(step):
        other = lax.rem(spot + step, line_size)
        return (quad * highs + other // blocks, lax.rem(other, blocks))

    def shifted(step):
        return lax.rem(slab + step + slabs, slabs)

    barrier = pltpu.get_barrier_semaphore()

    @pl.loop(1, quads)
    def _(step):
        pl.semaphore_signal(barrier, inc=1, device_id=plane_peer(step), device_id_type=MESH)

    @pl.loop(1, line_size)
    def _(step):
        pl.semaphore_signal(barrier, inc=1, device_id=line_peer(step), device_id_type=MESH)

    for step in (-1, 1):
        for side in (0, 1):
            pl.semaphore_signal(
                barrier, inc=1, device_id=(shifted(step), side * 2 + core), device_id_type=MESH
            )
    greeted = quads - 1 + line_size - 1 + 4

    even = (lax.broadcasted_iota(jnp.int32, (wide, 128), 0) % 2) == 0

    def make_piece(turn, source):
        for sphere in range(spheres):
            for part in range(2):
                stage_ref[0, pl.ds((2 * sphere + part) * rows, rows), :] = source[
                    pl.ds(sphere * wide + part, rows, stride=2), :
                ]
        piece_ref[turn] = stage_ref[0].astype(jnp.bfloat16)

    def send(src, dst, sems, slot, device):
        return pltpu.make_async_remote_copy(
            src_ref=src,
            dst_ref=dst,
            send_sem=send_sem.at[slot],
            recv_sem=sems,
            device_id=device,
            device_id_type=MESH,
        )

    def halo_copies(turn):
        own = piece_ref.at[turn]
        out = []
        slot = 24 + 11 * turn
        for step, side in ((1, 0), (1, 1), (-1, 0), (-1, 1)):
            out.append(
                send(
                    own,
                    halo_ref.at[turn, 1 - step, blk],
                    halo_sem.at[turn, 1 - step, blk],
                    slot + len(out),
                    (shifted(step), side * 2 + core),
                )
            )
        for device in ((slab, (1 - low) * 2 + core), (slab, low * 2 + 1 - core)):
            out.append(
                send(
                    own,
                    halo_ref.at[turn, 1, blk],
                    halo_sem.at[turn, 1, blk],
                    slot + len(out),
                    device,
                )
            )
        return out

    def forward_copies(turn):
        out = []
        slot = 30 + 11 * turn
        for place, side in ((1, 1 - low), (0, 0), (0, 1), (2, 0), (2, 1)):
            index = side * 2 + core
            out.append(
                send(
                    halo_ref.at[turn, place, index],
                    halo_ref.at[turn, place, index],
                    halo_sem.at[turn, place, index],
                    slot + len(out),
                    (slab, low * 2 + 1 - core),
                )
            )
        return out

    def exchange(src_of, dst, turn_slot, peer, size):
        @pl.loop(1, size)
        def _(step):
            send(src_of(step), dst, recv_sem.at[turn_slot], turn_slot, peer(step)).start()

    def drain(block, turn_slot, size, what):
        ref = block.at[pl.ds(0, size - 1)]
        copy = send(ref, ref, recv_sem.at[turn_slot], turn_slot, (slab, blk))
        if what == "recv":
            copy.wait_recv()
        else:
            copy.wait_send()

    def project(field):
        rounded = jnp.concatenate(
            [
                field[sphere * wide : (sphere + 1) * wide].astype(jnp.bfloat16)
                for sphere in range(spheres)
            ],
            axis=1,
        )
        product = jnp.dot(gather_ref[...], rounded, preferred_element_type=jnp.float32)
        sum_re = jnp.zeros((waves, 128), jnp.float32)
        sum_im = jnp.zeros((waves, 128), jnp.float32)
        for sphere in range(spheres):
            lanes = slice(128 * sphere, 128 * (sphere + 1))
            part_re = product[:waves, lanes]
            part_im = product[waves:, lanes]
            cos_part = trig_ref[:, sphere : sphere + 1]
            sin_part = trig_ref[:, spheres + sphere : spheres + sphere + 1]
            sum_re = sum_re + cos_part * part_re + sin_part * part_im
            sum_im = sum_im + cos_part * part_im - sin_part * part_re
        return sum_re, sum_im

    def cut(turn, sums):
        shards = waves // ROWS
        for part in range(2):
            cut_ref[turn, pl.ds(part * shards, shards)] = (
                sums[part].astype(jnp.bfloat16).reshape(shards, ROWS, 128)
            )

    shard_count = 2 * waves // ROWS
    per_device = shard_count // quads

    def shards_of(ref, turn, owner):
        return ref.at[turn, pl.ds(owner * per_device, per_device)]

    def start_scatter(turn):
        exchange(
            lambda step: shards_of(cut_ref, turn, lax.rem(quad + step, quads)),
            part_ref.at[turn, quad],
            10 * turn + 2,
            plane_peer,
            quads,
        )

    def finish_scatter(turn):
        part_ref[turn, quad] = cut_ref[turn, pl.ds(quad * per_device, per_device)]
        drain(part_ref.at[turn], 10 * turn + 2, quads, "recv")
        value = part_ref[turn].astype(jnp.float32).sum(axis=0)
        line_ref[turn, spot] = value.astype(jnp.bfloat16)

    def start_line(turn):
        exchange(
            lambda step: line_ref.at[turn, spot],
            line_ref.at[turn, spot],
            10 * turn + 3,
            line_peer,
            line_size,
        )

    def finish_line(turn):
        drain(line_ref.at[turn], 10 * turn + 3, line_size, "recv")
        value = line_ref[turn].astype(jnp.float32).sum(axis=0)
        sums_ref[turn, pl.ds(quad * per_device, per_device)] = value.astype(jnp.bfloat16)

    def start_gather(turn):
        exchange(
            lambda step: shards_of(sums_ref, turn, quad),
            shards_of(sums_ref, turn, quad),
            10 * turn + 4,
            plane_peer,
            quads,
        )

    def finish_gather(turn):
        ref = sums_ref.at[turn, pl.ds(0, (quads - 1) * per_device)]
        send(ref, ref, recv_sem.at[10 * turn + 4], 10 * turn + 4, (slab, blk)).wait_recv()

    def far_field(turn):
        shards = waves // ROWS
        sum_re = sums_ref[turn, pl.ds(0, shards)].astype(jnp.float32).reshape(waves, 128)
        sum_im = sums_ref[turn, pl.ds(shards, shards)].astype(jnp.float32).reshape(waves, 128)
        weight = trig_ref[:, 2 * spheres : 2 * spheres + 1]
        turned_re, turned_im = [], []
        for sphere in range(spheres):
            cos_part = weight * trig_ref[:, sphere : sphere + 1]
            sin_part = weight * trig_ref[:, spheres + sphere : spheres + sphere + 1]
            turned_re.append((cos_part * sum_re - sin_part * sum_im).astype(jnp.bfloat16))
            turned_im.append((cos_part * sum_im + sin_part * sum_re).astype(jnp.bfloat16))
        turned = jnp.concatenate(
            [jnp.concatenate(turned_re, axis=1), jnp.concatenate(turned_im, axis=1)], axis=0
        )
        return jnp.dot(spread_ref[...], turned, preferred_element_type=jnp.float32)

    def join(turn, place):
        for index in range(blocks):
            stage_ref[index] = halo_ref[turn, place, index].astype(jnp.float32)
        for sphere in range(spheres):
            for part in range(2):
                for index in range(blocks):
                    join_ref[
                        pl.ds(index * rows, rows), pl.ds(128 * part, 128)
                    ] = stage_ref[index, pl.ds((2 * sphere + part) * rows, rows), :]
            joined_ref[place * spheres + sphere] = join_ref[...].astype(jnp.bfloat16)

    def near_field(sphere):
        total_product = jnp.zeros((wide, 256), jnp.float32)
        for pair in range(pairs):
            number = sphere * pairs + pair
            total_product = total_product + jnp.dot(
                trans_ref[number],
                joined_ref[source_ref[number]],
                preferred_element_type=jnp.float32,
            )
        swapped = pair_swap(total_product[:, 128:], even)
        near_ref[pl.ds(sphere * wide, wide), :] = total_product[:, :128] + jnp.where(
            even, -swapped, swapped
        )

    def operator(turn, source, sums):
        cut(turn, sums)
        start_scatter(turn)
        halo = halo_copies(turn)
        for copy in halo:
            copy.start()
        halo_ref[turn, 1, blk] = piece_ref[turn]
        finish_scatter(turn)
        start_line(turn)
        forward = forward_copies(turn)
        for copy in forward:
            copy.wait_recv()
            copy.start()
        other = 1 - core

        def arrived(place, side):
            index = side * 2 + other
            send(
                halo_ref.at[turn, place, index],
                halo_ref.at[turn, place, index],
                halo_sem.at[turn, place, index],
                10 * turn + 1,
                (slab, blk),
            ).wait_recv()

        finish_line(turn)
        start_gather(turn)
        for place in (1, 0, 2):
            for side in (0, 1):
                arrived(place, side)
            join(turn, place)
        for sphere in range(spheres):
            near_field(sphere)
        finish_gather(turn)
        far = far_field(turn)
        out = []
        for sphere in range(spheres):
            span = slice(sphere * wide, (sphere + 1) * wide)
            summed = near_ref[span] + far[:, 128 * sphere : 128 * (sphere + 1)]
            swapped = pair_swap(summed, even)
            out.append(mie_ref[span, 0:1] * summed + mie_ref[span, 1:2] * swapped)
        return out, halo, forward

    start = [start_ref[sphere * wide : (sphere + 1) * wide] for sphere in range(spheres)]
    make_piece(0, start_ref)
    first_sums = project(start_ref[...])
    pl.semaphore_wait(barrier, greeted)
    image, halo_one, forward_one = operator(0, start_ref, first_sums)

    def put_gram(slot, pairs_of):
        lines = []
        for name, left, right in pairs_of:
            real, imag = 0.0, 0.0
            for sphere in range(spheres):
                swapped = pair_swap(right[sphere], even)
                part_re, part_im = inner_rows(left[sphere], right[sphere], swapped, even)
                real, imag = real + part_re, imag + part_im
            lines.append(real)
            if name == "complex":
                lines.append(imag)
        lines.append(jnp.zeros((8 - len(lines), 128), jnp.float32))
        gram_ref[slot, spot] = jnp.concatenate(lines, axis=0)

    def start_gram(slot, turn_slot):
        exchange(
            lambda step: gram_ref.at[slot, spot],
            gram_ref.at[slot, spot],
            turn_slot,
            line_peer,
            line_size,
        )

    def turn_gram(slot, turn_slot):
        ref = gram_ref.at[slot, pl.ds(0, line_size - 1)]
        send(ref, ref, recv_sem.at[turn_slot], turn_slot, (slab, blk)).wait_recv()
        gram_ref[slot + 1, quad] = gram_ref[slot, pl.ds(0, line_size)].sum(axis=0)
        exchange(
            lambda step: gram_ref.at[slot + 1, quad],
            gram_ref.at[slot + 1, quad],
            turn_slot + 1,
            plane_peer,
            quads,
        )

    def end_gram(slot, turn_slot):
        ref = gram_ref.at[slot + 1, pl.ds(0, quads - 1)]
        send(ref, ref, recv_sem.at[turn_slot + 1], turn_slot + 1, (slab, blk)).wait_recv()
        return gram_ref[slot + 1, pl.ds(0, quads)].sum(axis=0)

    for sphere in range(spheres):
        next_ref[pl.ds(sphere * wide, wide), :] = image[sphere]
    make_piece(1, next_ref)
    second_sums = project(next_ref[...])
    put_gram(0, (("real", start, start), ("complex", start, image), ("real", image, image)))
    start_gram(0, 20)
    second, halo_two, forward_two = operator(1, next_ref, second_sums)
    put_gram(2, (("complex", start, second), ("complex", image, second), ("real", second, second)))
    start_gram(2, 22)
    turn_gram(0, 20)
    turn_gram(2, 22)
    early = end_gram(0, 20)
    late = end_gram(2, 22)

    norm_start = early[0:1]
    c_re, c_im = early[1:2], early[2:3]
    norm_image = early[3:4]
    d_re, d_im = late[0:1], late[1:2]
    e_re, e_im = late[2:3], late[3:4]
    norm_second = late[4:5]
    shift = entries * epsilon
    whole = norm_start + shift
    beta = jnp.sqrt(whole / entries)
    h11_re, h11_im = (norm_start - c_re) / whole, -c_im / whole
    g_re, g_im = (shift + c_re) / whole, c_im / whole
    apart = norm_image - (
        2.0 * (g_re * c_re + g_im * c_im) - (g_re * g_re + g_im * g_im) * norm_start
    )
    h21 = jnp.sqrt(jnp.maximum(apart, 0.0) / whole + epsilon)
    scale = 1.0 / (beta * h21)
    a_re, a_im = g_re * scale, g_im * scale
    both = shift / whole * scale / beta
    q_re, q_im = both * (norm_start - c_re), -both * c_im
    over = scale / beta
    gc_re, gc_im = g_re * c_re - g_im * c_im, g_re * c_im + g_im * c_re
    h12_re = (q_re + over * (d_re - gc_re)) / entries
    h12_im = (q_im + over * (d_im - gc_im)) / entries
    u_re = a_re * c_re + a_im * c_im - scale * norm_image
    u_im = a_re * c_im - a_im * c_re
    v_re = a_re * d_re + a_im * d_im - scale * e_re
    v_im = a_re * d_im - a_im * d_re - scale * e_im
    k_re = a_re * u_re - a_im * u_im - scale * v_re + h12_re * q_re + h12_im * q_im
    k_im = a_re * u_im + a_im * u_re - scale * v_im + h12_im * q_re - h12_re * q_im
    kap_re = epsilon / (h21 * h21) + k_re / entries
    kap_im = k_im / entries
    h22_re, h22_im = 1.0 - kap_re, -kap_im
    x_re = a_re * kap_re - a_im * kap_im - h12_re / beta
    x_im = a_re * kap_im + a_im * kap_re - h12_im / beta
    y_re = -scale * kap_re - a_re
    y_im = -scale * kap_im - a_im
    xy_re, xy_im = x_re * y_re + x_im * y_im, x_re * y_im - x_im * y_re
    left = (
        (x_re * x_re + x_im * x_im) * norm_start
        + (y_re * y_re + y_im * y_im) * norm_image
        + scale * scale * norm_second
        + 2.0 * (xy_re * c_re - xy_im * c_im)
        + 2.0 * scale * (x_re * d_re + x_im * d_im)
        + 2.0 * scale * (y_re * e_re + y_im * e_im)
    )
    h32 = jnp.sqrt(jnp.maximum(left, 0.0) / entries + epsilon)
    hess_ref[...] = jnp.concatenate(
        [
            beta,
            h11_re,
            h11_im,
            h21,
            h12_re,
            h12_im,
            h22_re,
            h22_im,
            h32,
            jnp.zeros((7, 128), jnp.float32),
        ],
        axis=0,
    )
    for sphere in range(spheres):
        span = pl.ds(sphere * wide, wide)
        one = start_ref[span, :]
        two = next_ref[span, :]
        one_swapped, two_swapped = pair_swap(one, even), pair_swap(two, even)
        residual_ref[span, :] = (
            complex_rows(x_re, x_im, one, one_swapped, even)
            + complex_rows(y_re, y_im, two, two_swapped, even)
            + scale * second[sphere]
        )
        next_ref[span, :] = complex_rows(a_re, a_im, one, one_swapped, even) - scale * two

    for copy in halo_one + forward_one + halo_two + forward_two:
        copy.wait_send()
    for turn in range(2):
        for slot, size, block in (
            (2, quads, part_ref.at[turn]),
            (3, line_size, line_ref.at[turn]),
            (4, quads, part_ref.at[turn]),
        ):
            drain(block, 10 * turn + slot, size, "send")
    for slot in (0, 2):
        drain(gram_ref.at[slot], 20 + slot, line_size, "send")
        drain(gram_ref.at[slot + 1], 21 + slot, quads, "send")


def per_device(
    quads,
    highs,
    incident,
    mie_coef,
    translation,
    pair_shift,
    pair_member,
    positions,
    wave_index,
    plane_coef,
    ewald_weight,
):
    spheres, _, rows, fields = incident.shape
    pairs = translation.shape[1]
    coefs = translation.shape[4]
    waves = plane_coef.shape[0]
    total = spheres * 2 * rows
    entries = quads * highs * spheres * coefs
    blocks = coefs // rows
    line_size = highs * blocks
    start = incident.transpose(0, 2, 1, 3).reshape(total, fields)
    trans = translation.transpose(0, 1, 3, 2, 4).reshape(spheres * pairs, 2 * rows, coefs)
    sources = ((pair_shift + 1) * spheres + pair_member).reshape(-1)
    angles = two_pi * jnp.sum(
        wave_index.astype(jnp.float32)[:, None, :] * positions[None, :, :], axis=-1
    )
    trig = jnp.concatenate([jnp.cos(angles), jnp.sin(angles), ewald_weight[:, None]], axis=1)
    mie_re = jnp.repeat(mie_coef[:, 0].reshape(-1), 2)
    mie_im = jnp.stack([-mie_coef[:, 1], mie_coef[:, 1]], axis=-1).reshape(-1)
    mie = jnp.stack([mie_re, mie_im], axis=1)
    coef_rows = lax.dynamic_slice_in_dim(plane_coef, lax.axis_index(BLK) * rows, rows, 2)
    coef_re, coef_im = coef_rows[:, 0].T, coef_rows[:, 1].T
    spread = jnp.stack(
        [
            jnp.concatenate([coef_re, coef_im], axis=1),
            jnp.concatenate([-coef_im, coef_re], axis=1),
        ],
        axis=1,
    ).reshape(2 * rows, 2 * waves)
    gather = spread.T
    shard_count = 2 * waves // ROWS
    per_quad = shard_count // quads
    vmem = pl.BlockSpec(memory_space=pltpu.VMEM)
    basis, residual, hess = pl.pallas_call(
        functools.partial(kernel, quads, highs, spheres, pairs, coefs, entries),
        out_shape=(
            jax.ShapeDtypeStruct((total, fields), jnp.float32),
            jax.ShapeDtypeStruct((total, fields), jnp.float32),
            jax.ShapeDtypeStruct((16, fields), jnp.float32),
        ),
        in_specs=[pl.BlockSpec(memory_space=pltpu.SMEM)] + [vmem] * 6,
        out_specs=(vmem, vmem, vmem),
        scratch_shapes=[
            pltpu.VMEM((2, total, fields), jnp.bfloat16),
            pltpu.VMEM((2, 3, blocks, total, fields), jnp.bfloat16),
            pltpu.VMEM((blocks, total, fields), jnp.float32),
            pltpu.VMEM((coefs, 2 * fields), jnp.float32),
            pltpu.VMEM((3 * spheres, coefs, 2 * fields), jnp.bfloat16),
            pltpu.VMEM((2, shard_count, ROWS, fields), jnp.bfloat16),
            pltpu.VMEM((2, quads, per_quad, ROWS, fields), jnp.bfloat16),
            pltpu.VMEM((2, line_size, per_quad, ROWS, fields), jnp.bfloat16),
            pltpu.VMEM((2, shard_count, ROWS, fields), jnp.bfloat16),
            pltpu.VMEM((4, max(quads, line_size), 8, fields), jnp.float32),
            pltpu.VMEM((total, fields), jnp.float32),
            pltpu.SemaphoreType.DMA((46,)),
            pltpu.SemaphoreType.DMA((24,)),
            pltpu.SemaphoreType.DMA((2, 3, blocks)),
        ],
        compiler_params=pltpu.CompilerParams(collective_id=0, has_side_effects=True),
        name="arnoldi",
    )(sources, start, gather, spread, trig, mie, trans)

    def unpacked(field):
        return field.reshape(spheres, rows, 2, fields).transpose(0, 2, 1, 3)

    return unpacked(basis), unpacked(residual), hess[:9]


def solution(mesh):
    highs = 4 if mesh.shape[SLAB] % 4 == 0 and mesh.shape[SLAB] > 4 else 2
    quads = mesh.shape[SLAB] // highs
    return jax.shard_map(
        functools.partial(per_device, quads, highs),
        mesh=mesh,
        in_specs=(
            P(SLAB, None, BLK, None),
            P(SLAB, None, BLK),
            P(SLAB, None, None, BLK, None),
            P(SLAB, None),
            P(SLAB, None),
            P(SLAB, None),
            P(),
            P(),
            P(),
        ),
        out_specs=(P(SLAB, None, BLK, None), P(SLAB, None, BLK, None), P()),
        check_vma=False,
    )
```

```python
import functools

import jax
import jax.numpy as jnp
from jax import lax
from jax.experimental import pallas as pl
from jax.experimental.pallas import tpu as pltpu
from jax.sharding import PartitionSpec as P

MESH = pl.DeviceIdType.MESH
SLAB = "slab"
BLK = "blk"
two_pi = 6.283185307179586
epsilon = 1e-06

ROWS = 16


def pair_swap(field, even):
    count = field.shape[0]
    return jnp.where(even, pltpu.roll(field, count - 1, 0), pltpu.roll(field, 1, 0))


def complex_rows(coef_re, coef_im, field, swapped, even):
    return coef_re * field + jnp.where(even, -coef_im, coef_im) * swapped


def inner_rows(left, right, right_swapped, even):
    real = jnp.sum(left * right, axis=0, keepdims=True)
    cross = left * right_swapped
    imag = jnp.sum(jnp.where(even, cross, -cross), axis=0, keepdims=True)
    return real, imag


def kernel(
    quads,
    highs,
    spheres,
    pairs,
    coefs,
    entries,
    shift_ref,
    member_ref,
    position_ref,
    wave_ref,
    weight_ref,
    mie_in_ref,
    start_hbm,
    plane_hbm,
    trans_hbm,
    image_hbm,
    second_hbm,
    out_ref,
    start_ref,
    plane_ref,
    trans_ref,
    gather_ref,
    spread_ref,
    trig_ref,
    mie_ref,
    image_ref,
    second_ref,
    piece_ref,
    halo_ref,
    stage_ref,
    join_ref,
    joined_ref,
    cut_ref,
    part_ref,
    line_ref,
    sums_ref,
    gram_ref,
    near_ref,
    send_sem,
    recv_sem,
    halo_sem,
    load_sem,
):
    blocks = 4
    slabs = quads * highs
    line_size = highs * blocks
    slab = lax.axis_index(SLAB)
    blk = lax.axis_index(BLK)
    quad = slab // highs
    high = slab % highs
    core = blk % 2
    low = blk // 2
    spot = high * blocks + blk
    rows = coefs // blocks
    wide = 2 * rows
    total = spheres * wide
    waves = gather_ref.shape[0] // 2
    loads = [
        pltpu.make_async_copy(src, dst, load_sem.at[number])
        for number, (src, dst) in enumerate(
            ((plane_hbm, plane_ref), (start_hbm, start_ref), (trans_hbm, trans_ref))
        )
    ]
    for load in loads:
        load.start()

    def far_first(step, size):
        half = (step + 1) // 2
        return lax.rem(size // 2 + jnp.where(lax.rem(step, 2) == 1, -half, half), size)

    ring_x = 4 if quads == 32 else 1
    ring_z = quads // ring_x

    def plane_quad(step):
        place_x = lax.rem(quad // ring_z + far_first(lax.rem(step, ring_x), ring_x), ring_x)
        place_z = lax.rem(lax.rem(quad, ring_z) + far_first(step // ring_x, ring_z), ring_z)
        return place_x * ring_z + place_z

    def plane_peer(step):
        return (plane_quad(step) * highs + high, blk)

    def line_peer(step):
        place = lax.rem(2 * high + low + far_first(step // 2, 2 * highs), 2 * highs)
        side = lax.rem(core + 1 - lax.rem(step, 2), 2)
        return (quad * highs + place // 2, lax.rem(place, 2) * 2 + side)

    def shifted(step):
        return lax.rem(slab + step + slabs, slabs)

    barrier = pltpu.get_barrier_semaphore()

    @pl.loop(0, quads - 1)
    def _(step):
        pl.semaphore_signal(barrier, inc=1, device_id=plane_peer(step), device_id_type=MESH)

    @pl.loop(0, line_size - 1)
    def _(step):
        pl.semaphore_signal(barrier, inc=1, device_id=line_peer(step), device_id_type=MESH)

    for step in (-1, 1):
        for side in (0, 1):
            pl.semaphore_signal(
                barrier, inc=1, device_id=(shifted(step), side * 2 + core), device_id_type=MESH
            )
    greeted = quads - 1 + line_size - 1 + 4

    even = (lax.broadcasted_iota(jnp.int32, (wide, 128), 0) % 2) == 0

    def make_piece(turn, source):
        for sphere in range(spheres):
            for part in range(2):
                stage_ref[0, pl.ds((2 * sphere + part) * rows, rows), :] = source[
                    pl.ds(sphere * wide + part, rows, stride=2), :
                ]
        piece_ref[turn] = stage_ref[0].astype(jnp.bfloat16)

    def send(src, dst, sems, slot, device):
        return pltpu.make_async_remote_copy(
            src_ref=src,
            dst_ref=dst,
            send_sem=send_sem.at[slot],
            recv_sem=sems,
            device_id=device,
            device_id_type=MESH,
        )

    def halo_copies(turn):
        own = piece_ref.at[turn]
        out = []
        slot = 24 + 11 * turn
        for step, side in ((1, 1), (-1, 0), (1, 0), (-1, 1)):
            out.append(
                send(
                    own,
                    halo_ref.at[turn, 1 - step, blk],
                    halo_sem.at[turn, 1 - step, blk],
                    slot + len(out),
                    (shifted(step), side * 2 + core),
                )
            )
        for device in ((slab, (1 - low) * 2 + core), (slab, low * 2 + 1 - core)):
            out.append(
                send(
                    own,
                    halo_ref.at[turn, 1, blk],
                    halo_sem.at[turn, 1, blk],
                    slot + len(out),
                    device,
                )
            )
        return out

    def forward_copies(turn):
        out = []
        slot = 30 + 11 * turn
        for place, side in ((1, 1 - low), (0, 0), (0, 1), (2, 0), (2, 1)):
            index = side * 2 + core
            out.append(
                send(
                    halo_ref.at[turn, place, index],
                    halo_ref.at[turn, place, index],
                    halo_sem.at[turn, place, index],
                    slot + len(out),
                    (slab, low * 2 + 1 - core),
                )
            )
        return out

    def exchange(src_of, dst, turn_slot, peer, size):
        @pl.loop(0, size - 1)
        def _(step):
            send(src_of(step), dst, recv_sem.at[turn_slot], turn_slot, peer(step)).start()

    def drain(block, turn_slot, size, what):
        ref = block.at[pl.ds(0, size - 1)]
        copy = send(ref, ref, recv_sem.at[turn_slot], turn_slot, (slab, blk))
        if what == "recv":
            copy.wait_recv()
        else:
            copy.wait_send()

    def project(field):
        rounded = jnp.concatenate(
            [
                field[sphere * wide : (sphere + 1) * wide].astype(jnp.bfloat16)
                for sphere in range(spheres)
            ],
            axis=1,
        )
        product = jnp.dot(gather_ref[...], rounded, preferred_element_type=jnp.float32)
        sum_re = jnp.zeros((waves, 128), jnp.float32)
        sum_im = jnp.zeros((waves, 128), jnp.float32)
        for sphere in range(spheres):
            lanes = slice(128 * sphere, 128 * (sphere + 1))
            part_re = product[:waves, lanes]
            part_im = product[waves:, lanes]
            cos_part = trig_ref[:, sphere : sphere + 1]
            sin_part = trig_ref[:, spheres + sphere : spheres + sphere + 1]
            sum_re = sum_re + cos_part * part_re + sin_part * part_im
            sum_im = sum_im + cos_part * part_im - sin_part * part_re
        return sum_re, sum_im

    def cut(turn, sums):
        shards = waves // ROWS
        for part in range(2):
            cut_ref[turn, pl.ds(part * shards, shards)] = (
                sums[part].astype(jnp.bfloat16).reshape(shards, ROWS, 128)
            )

    shard_count = 2 * waves // ROWS
    per_device = shard_count // quads

    def shards_of(ref, turn, owner):
        return ref.at[turn, pl.ds(owner * per_device, per_device)]

    def start_scatter(turn):
        exchange(
            lambda step: shards_of(cut_ref, turn, plane_quad(step)),
            part_ref.at[turn, quad],
            10 * turn + 2,
            plane_peer,
            quads,
        )

    def finish_scatter(turn):
        part_ref[turn, quad] = cut_ref[turn, pl.ds(quad * per_device, per_device)]
        drain(part_ref.at[turn], 10 * turn + 2, quads, "recv")
        value = part_ref[turn].astype(jnp.float32).sum(axis=0)
        line_ref[turn, spot] = value.astype(jnp.bfloat16)

    def start_line(turn):
        exchange(
            lambda step: line_ref.at[turn, spot],
            line_ref.at[turn, spot],
            10 * turn + 3,
            line_peer,
            line_size,
        )

    def finish_line(turn):
        drain(line_ref.at[turn], 10 * turn + 3, line_size, "recv")
        value = line_ref[turn].astype(jnp.float32).sum(axis=0)
        sums_ref[turn, pl.ds(quad * per_device, per_device)] = value.astype(jnp.bfloat16)

    def start_gather(turn):
        exchange(
            lambda step: shards_of(sums_ref, turn, quad),
            shards_of(sums_ref, turn, quad),
            10 * turn + 4,
            plane_peer,
            quads,
        )

    def finish_gather(turn):
        ref = sums_ref.at[turn, pl.ds(0, (quads - 1) * per_device)]
        send(ref, ref, recv_sem.at[10 * turn + 4], 10 * turn + 4, (slab, blk)).wait_recv()

    def far_field(turn):
        shards = waves // ROWS
        sum_re = sums_ref[turn, pl.ds(0, shards)].astype(jnp.float32).reshape(waves, 128)
        sum_im = sums_ref[turn, pl.ds(shards, shards)].astype(jnp.float32).reshape(waves, 128)
        weight = trig_ref[:, 2 * spheres : 2 * spheres + 1]
        turned_re, turned_im = [], []
        for sphere in range(spheres):
            cos_part = weight * trig_ref[:, sphere : sphere + 1]
            sin_part = weight * trig_ref[:, spheres + sphere : spheres + sphere + 1]
            turned_re.append((cos_part * sum_re - sin_part * sum_im).astype(jnp.bfloat16))
            turned_im.append((cos_part * sum_im + sin_part * sum_re).astype(jnp.bfloat16))
        turned = jnp.concatenate(
            [jnp.concatenate(turned_re, axis=1), jnp.concatenate(turned_im, axis=1)], axis=0
        )
        return jnp.dot(spread_ref[...], turned, preferred_element_type=jnp.float32)

    def join(turn, place):
        for index in range(blocks):
            stage_ref[index] = halo_ref[turn, place, index].astype(jnp.float32)
        for sphere in range(spheres):
            for part in range(2):
                for index in range(blocks):
                    join_ref[
                        pl.ds(index * rows, rows), pl.ds(128 * part, 128)
                    ] = stage_ref[index, pl.ds((2 * sphere + part) * rows, rows), :]
            joined_ref[place * spheres + sphere] = join_ref[...].astype(jnp.bfloat16)

    def near_field(sphere):
        total_product = jnp.zeros((wide, 256), jnp.float32)
        for pair in range(pairs):
            number = sphere * pairs + pair
            source = (shift_ref[sphere, pair] + 1) * spheres + member_ref[sphere, pair]
            total_product = total_product + jnp.dot(
                trans_ref[number].reshape(wide, coefs),
                joined_ref[source],
                preferred_element_type=jnp.float32,
            )
        swapped = pair_swap(total_product[:, 128:], even)
        near_ref[pl.ds(sphere * wide, wide), :] = total_product[:, :128] + jnp.where(
            even, -swapped, swapped
        )

    def operator(turn, source, sums):
        cut(turn, sums)
        start_scatter(turn)
        halo = halo_copies(turn)
        for copy in halo:
            copy.start()
        halo_ref[turn, 1, blk] = piece_ref[turn]
        finish_scatter(turn)
        start_line(turn)
        forward = forward_copies(turn)
        for copy in forward:
            copy.wait_recv()
            copy.start()
        other = 1 - core

        def arrived(place, side):
            index = side * 2 + other
            send(
                halo_ref.at[turn, place, index],
                halo_ref.at[turn, place, index],
                halo_sem.at[turn, place, index],
                10 * turn + 1,
                (slab, blk),
            ).wait_recv()

        finish_line(turn)
        start_gather(turn)
        for place in (1, 0, 2):
            for side in (0, 1):
                arrived(place, side)
            join(turn, place)
        if turn == 0:
            loads[2].wait()
        for sphere in range(spheres):
            near_field(sphere)
        if turn == 0:
            spread_mie()
        finish_gather(turn)
        far = far_field(turn)
        out = []
        for sphere in range(spheres):
            span = slice(sphere * wide, (sphere + 1) * wide)
            summed = near_ref[span] + far[:, 128 * sphere : 128 * (sphere + 1)]
            swapped = pair_swap(summed, even)
            out.append(mie_ref[0, span] * summed + mie_ref[1, span] * swapped)
        return out, halo, forward

    def make_trig():
        cos_rows, sin_rows = [], []
        for sphere in range(spheres):
            turns = jnp.zeros((1, waves), jnp.float32)
            for axis in range(3):
                turns = turns + wave_ref[axis : axis + 1, :].astype(jnp.float32) * (
                    position_ref[sphere, axis]
                )
            angle = two_pi * (turns - jnp.round(turns))
            cos_rows.append(jnp.cos(angle))
            sin_rows.append(jnp.sin(angle))
        lines = cos_rows + sin_rows + [weight_ref[...]]
        lines.append(jnp.zeros((128 - len(lines), waves), jnp.float32))
        trig_ref[...] = jnp.concatenate(lines, axis=0).T

    def make_plane():
        upper = jnp.concatenate([plane_ref[0], plane_ref[1]], axis=1)
        lower = jnp.concatenate([-plane_ref[1], plane_ref[0]], axis=1)
        row = lax.broadcasted_iota(jnp.int32, (wide, coefs), 0)
        hit = lax.broadcasted_iota(jnp.int32, (wide, coefs), 1) == blk * rows + row // 2
        real = jnp.where(hit & (row % 2 == 0), 1.0, 0.0).astype(jnp.bfloat16)
        imag = jnp.where(hit & (row % 2 == 1), 1.0, 0.0).astype(jnp.bfloat16)
        own = jnp.dot(real, upper, preferred_element_type=jnp.float32) + jnp.dot(
            imag, lower, preferred_element_type=jnp.float32
        )
        spread_ref[...] = own.astype(jnp.bfloat16)
        gather_ref[...] = own.T.astype(jnp.bfloat16)

    def spread_mie():
        lines = jnp.concatenate(
            [mie_in_ref[sphere] for sphere in range(spheres)]
            + [jnp.zeros((128 - 2 * spheres, rows), jnp.float32)],
            axis=0,
        )
        lines = jnp.concatenate([lines, jnp.zeros((128, 128 - rows), jnp.float32)], axis=1).T
        for sphere in range(spheres):
            real = jnp.broadcast_to(lines[:rows, 2 * sphere : 2 * sphere + 1], (rows, 128))
            imag = jnp.broadcast_to(lines[:rows, 2 * sphere + 1 : 2 * sphere + 2], (rows, 128))
            base = sphere * wide
            mie_ref[0, pl.ds(base, rows, stride=2), :] = real
            mie_ref[0, pl.ds(base + 1, rows, stride=2), :] = real
            mie_ref[1, pl.ds(base, rows, stride=2), :] = -imag
            mie_ref[1, pl.ds(base + 1, rows, stride=2), :] = imag

    make_trig()
    loads[0].wait()
    make_plane()
    loads[1].wait()
    start = [start_ref[sphere * wide : (sphere + 1) * wide] for sphere in range(spheres)]
    make_piece(0, start_ref)
    first_sums = project(start_ref[...])
    pl.semaphore_wait(barrier, greeted)
    image, halo_one, forward_one = operator(0, start_ref, first_sums)

    def put_gram(slot, pairs_of):
        lines = []
        for name, left, right in pairs_of:
            real, imag = 0.0, 0.0
            for sphere in range(spheres):
                swapped = pair_swap(right[sphere], even)
                part_re, part_im = inner_rows(left[sphere], right[sphere], swapped, even)
                real, imag = real + part_re, imag + part_im
            lines.append(real)
            if name == "complex":
                lines.append(imag)
        lines.append(jnp.zeros((8 - len(lines), 128), jnp.float32))
        gram_ref[slot, spot] = jnp.concatenate(lines, axis=0)

    def start_gram(slot, turn_slot):
        exchange(
            lambda step: gram_ref.at[slot, spot],
            gram_ref.at[slot, spot],
            turn_slot,
            line_peer,
            line_size,
        )

    def turn_gram(slot, turn_slot):
        ref = gram_ref.at[slot, pl.ds(0, line_size - 1)]
        send(ref, ref, recv_sem.at[turn_slot], turn_slot, (slab, blk)).wait_recv()
        gram_ref[slot + 1, quad] = gram_ref[slot, pl.ds(0, line_size)].sum(axis=0)
        exchange(
            lambda step: gram_ref.at[slot + 1, quad],
            gram_ref.at[slot + 1, quad],
            turn_slot + 1,
            plane_peer,
            quads,
        )

    def end_gram(slot, turn_slot):
        ref = gram_ref.at[slot + 1, pl.ds(0, quads - 1)]
        send(ref, ref, recv_sem.at[turn_slot + 1], turn_slot + 1, (slab, blk)).wait_recv()
        return gram_ref[slot + 1, pl.ds(0, quads)].sum(axis=0)

    for sphere in range(spheres):
        image_ref[pl.ds(sphere * wide, wide), :] = image[sphere]
    make_piece(1, image_ref)
    second_sums = project(image_ref[...])
    store_image = pltpu.make_async_copy(image_ref, image_hbm, load_sem.at[3])
    store_image.start()
    put_gram(0, (("real", start, start), ("complex", start, image), ("real", image, image)))
    start_gram(0, 20)
    second, halo_two, forward_two = operator(1, image_ref, second_sums)
    put_gram(2, (("complex", start, second), ("complex", image, second), ("real", second, second)))
    start_gram(2, 22)
    for sphere in range(spheres):
        second_ref[pl.ds(sphere * wide, wide), :] = second[sphere]
    store_second = pltpu.make_async_copy(second_ref, second_hbm, load_sem.at[4])
    store_second.start()
    turn_gram(0, 20)
    turn_gram(2, 22)
    early = end_gram(0, 20)
    late = end_gram(2, 22)

    norm_start = early[0:1]
    c_re, c_im = early[1:2], early[2:3]
    norm_image = early[3:4]
    d_re, d_im = late[0:1], late[1:2]
    e_re, e_im = late[2:3], late[3:4]
    norm_second = late[4:5]
    shift = entries * epsilon
    whole = norm_start + shift
    beta = jnp.sqrt(whole / entries)
    h11_re, h11_im = (norm_start - c_re) / whole, -c_im / whole
    g_re, g_im = (shift + c_re) / whole, c_im / whole
    apart = norm_image - (
        2.0 * (g_re * c_re + g_im * c_im) - (g_re * g_re + g_im * g_im) * norm_start
    )
    h21 = jnp.sqrt(jnp.maximum(apart, 0.0) / whole + epsilon)
    scale = 1.0 / (beta * h21)
    a_re, a_im = g_re * scale, g_im * scale
    both = shift / whole * scale / beta
    q_re, q_im = both * (norm_start - c_re), -both * c_im
    over = scale / beta
    gc_re, gc_im = g_re * c_re - g_im * c_im, g_re * c_im + g_im * c_re
    h12_re = (q_re + over * (d_re - gc_re)) / entries
    h12_im = (q_im + over * (d_im - gc_im)) / entries
    u_re = a_re * c_re + a_im * c_im - scale * norm_image
    u_im = a_re * c_im - a_im * c_re
    v_re = a_re * d_re + a_im * d_im - scale * e_re
    v_im = a_re * d_im - a_im * d_re - scale * e_im
    k_re = a_re * u_re - a_im * u_im - scale * v_re + h12_re * q_re + h12_im * q_im
    k_im = a_re * u_im + a_im * u_re - scale * v_im + h12_im * q_re - h12_re * q_im
    kap_re = epsilon / (h21 * h21) + k_re / entries
    kap_im = k_im / entries
    h22_re, h22_im = 1.0 - kap_re, -kap_im
    x_re = a_re * kap_re - a_im * kap_im - h12_re / beta
    x_im = a_re * kap_im + a_im * kap_re - h12_im / beta
    y_re = -scale * kap_re - a_re
    y_im = -scale * kap_im - a_im
    xy_re, xy_im = x_re * y_re + x_im * y_im, x_re * y_im - x_im * y_re
    left = (
        (x_re * x_re + x_im * x_im) * norm_start
        + (y_re * y_re + y_im * y_im) * norm_image
        + scale * scale * norm_second
        + 2.0 * (xy_re * c_re - xy_im * c_im)
        + 2.0 * scale * (x_re * d_re + x_im * d_im)
        + 2.0 * scale * (y_re * e_re + y_im * e_im)
    )
    h32 = jnp.sqrt(jnp.maximum(left, 0.0) / entries + epsilon)
    out_ref[...] = jnp.concatenate(
        [beta, h11_re, h11_im, h21, h12_re, h12_im, h22_re, h22_im, h32]
        + [a_re, a_im, x_re, x_im, y_re, y_im, scale, jnp.zeros((8, 128), jnp.float32)],
        axis=0,
    )
    store_image.wait()
    store_second.wait()

    for copy in halo_one + forward_one + halo_two + forward_two:
        copy.wait_send()
    for turn in range(2):
        for slot, size, block in (
            (2, quads, part_ref.at[turn]),
            (3, line_size, line_ref.at[turn]),
            (4, quads, part_ref.at[turn]),
        ):
            drain(block, 10 * turn + slot, size, "send")
    for slot in (0, 2):
        drain(gram_ref.at[slot], 20 + slot, line_size, "send")
        drain(gram_ref.at[slot + 1], 21 + slot, quads, "send")


def combine_kernel(
    spheres, scalar_ref, start_ref, image_ref, second_ref, next_ref, residual_ref, hess_ref
):
    wide = start_ref.shape[0] // spheres
    even = (lax.broadcasted_iota(jnp.int32, (wide, 128), 0) % 2) == 0
    hess_ref[...] = scalar_ref[0:9, :]
    a_re, a_im, x_re, x_im, y_re, y_im, scale = (
        scalar_ref[9 + number : 10 + number, :] for number in range(7)
    )
    for sphere in range(spheres):
        span = pl.ds(sphere * wide, wide)
        one = start_ref[span, :]
        two = image_ref[span, :]
        one_swapped, two_swapped = pair_swap(one, even), pair_swap(two, even)
        next_ref[span, :] = complex_rows(a_re, a_im, one, one_swapped, even) - scale * two
        residual_ref[span, :] = (
            complex_rows(x_re, x_im, one, one_swapped, even)
            + complex_rows(y_re, y_im, two, two_swapped, even)
            + scale * second_ref[span, :]
        )


def per_device(
    quads,
    highs,
    incident,
    mie_coef,
    translation,
    pair_shift,
    pair_member,
    positions,
    wave_index,
    plane_coef,
    ewald_weight,
):
    spheres, _, rows, fields = incident.shape
    pairs = translation.shape[1]
    coefs = translation.shape[4]
    waves = plane_coef.shape[0]
    total = spheres * 2 * rows
    entries = quads * highs * spheres * coefs
    blocks = coefs // rows
    line_size = highs * blocks
    start = incident.transpose(0, 2, 1, 3).reshape(total, fields)
    trans = translation.transpose(0, 1, 3, 2, 4).reshape(spheres * pairs, rows, 2, coefs)
    shard_count = 2 * waves // ROWS
    per_quad = shard_count // quads
    vmem = pl.BlockSpec(memory_space=pltpu.VMEM)
    smem = pl.BlockSpec(memory_space=pltpu.SMEM)
    hbm = pl.BlockSpec(memory_space=pl.ANY)
    vector = jax.ShapeDtypeStruct((total, fields), jnp.float32)
    image, second, scalars = pl.pallas_call(
        functools.partial(kernel, quads, highs, spheres, pairs, coefs, entries),
        out_shape=(vector, vector, jax.ShapeDtypeStruct((24, fields), jnp.float32)),
        in_specs=[smem, smem, smem, vmem, vmem, vmem, hbm, hbm, hbm],
        out_specs=(hbm, hbm, vmem),
        scratch_shapes=[
            pltpu.VMEM((total, fields), jnp.float32),
            pltpu.VMEM((2, coefs, waves), jnp.bfloat16),
            pltpu.VMEM((spheres * pairs, rows, 2, coefs), jnp.bfloat16),
            pltpu.VMEM((2 * waves, 2 * rows), jnp.bfloat16),
            pltpu.VMEM((2 * rows, 2 * waves), jnp.bfloat16),
            pltpu.VMEM((waves, 128), jnp.float32),
            pltpu.VMEM((2, total, fields), jnp.float32),
            pltpu.VMEM((total, fields), jnp.float32),
            pltpu.VMEM((total, fields), jnp.float32),
            pltpu.VMEM((2, total, fields), jnp.bfloat16),
            pltpu.VMEM((2, 3, blocks, total, fields), jnp.bfloat16),
            pltpu.VMEM((blocks, total, fields), jnp.float32),
            pltpu.VMEM((coefs, 2 * fields), jnp.float32),
            pltpu.VMEM((3 * spheres, coefs, 2 * fields), jnp.bfloat16),
            pltpu.VMEM((2, shard_count, ROWS, fields), jnp.bfloat16),
            pltpu.VMEM((2, quads, per_quad, ROWS, fields), jnp.bfloat16),
            pltpu.VMEM((2, line_size, per_quad, ROWS, fields), jnp.bfloat16),
            pltpu.VMEM((2, shard_count, ROWS, fields), jnp.bfloat16),
            pltpu.VMEM((4, max(quads, line_size), 8, fields), jnp.float32),
            pltpu.VMEM((total, fields), jnp.float32),
            pltpu.SemaphoreType.DMA((46,)),
            pltpu.SemaphoreType.DMA((24,)),
            pltpu.SemaphoreType.DMA((2, 3, blocks)),
            pltpu.SemaphoreType.DMA((5,)),
        ],
        compiler_params=pltpu.CompilerParams(collective_id=0, has_side_effects=True),
        name="arnoldi",
    )(
        pair_shift,
        pair_member,
        positions,
        wave_index.T,
        ewald_weight.reshape(1, waves),
        mie_coef,
        start,
        plane_coef.transpose(1, 2, 0),
        trans,
    )
    basis, residual, hess = pl.pallas_call(
        functools.partial(combine_kernel, spheres),
        out_shape=(vector, vector, jax.ShapeDtypeStruct((9, fields), jnp.float32)),
        in_specs=[vmem] * 4,
        out_specs=(vmem, vmem, vmem),
        name="combine",
    )(scalars, start, image, second)

    def unpacked(field):
        return field.reshape(spheres, rows, 2, fields).transpose(0, 2, 1, 3)

    return unpacked(basis), unpacked(residual), hess


def solution(mesh):
    highs = 4 if mesh.shape[SLAB] % 4 == 0 and mesh.shape[SLAB] > 4 else 2
    quads = mesh.shape[SLAB] // highs
    return jax.shard_map(
        functools.partial(per_device, quads, highs),
        mesh=mesh,
        in_specs=(
            P(SLAB, None, BLK, None),
            P(SLAB, None, BLK),
            P(SLAB, None, None, BLK, None),
            P(SLAB, None),
            P(SLAB, None),
            P(SLAB, None),
            P(),
            P(),
            P(),
        ),
        out_specs=(P(SLAB, None, BLK, None), P(SLAB, None, BLK, None), P()),
        check_vma=False,
    )
```

```python
import functools

import jax
import jax.numpy as jnp
from jax import lax
from jax.experimental import pallas as pl
from jax.experimental.pallas import tpu as pltpu
from jax.sharding import PartitionSpec as P

MESH = pl.DeviceIdType.MESH
SLAB = "slab"
BLK = "blk"
two_pi = 6.283185307179586
epsilon = 1e-06

ROWS = 16


def pair_swap(field, even):
    count = field.shape[0]
    return jnp.where(even, pltpu.roll(field, count - 1, 0), pltpu.roll(field, 1, 0))


def complex_rows(coef_re, coef_im, field, swapped, even):
    return coef_re * field + jnp.where(even, -coef_im, coef_im) * swapped


def inner_rows(left, right, right_swapped, even):
    real = jnp.sum(left * right, axis=0, keepdims=True)
    cross = left * right_swapped
    imag = jnp.sum(jnp.where(even, cross, -cross), axis=0, keepdims=True)
    return real, imag


def kernel(
    quads,
    highs,
    spheres,
    pairs,
    coefs,
    entries,
    shift_ref,
    member_ref,
    position_ref,
    wave_ref,
    weight_ref,
    mie_in_ref,
    start_hbm,
    plane_hbm,
    trans_hbm,
    start_ref,
    image_ref,
    second_ref,
    out_ref,
    plane_ref,
    trans_ref,
    gather_ref,
    spread_ref,
    trig_ref,
    mie_ref,
    piece_ref,
    halo_ref,
    stage_ref,
    join_ref,
    joined_ref,
    cut_ref,
    part_ref,
    line_ref,
    sums_ref,
    gram_ref,
    near_ref,
    send_sem,
    recv_sem,
    halo_sem,
    load_sem,
):
    blocks = 4
    slabs = quads * highs
    line_size = highs * blocks
    slab = lax.axis_index(SLAB)
    blk = lax.axis_index(BLK)
    quad = slab // highs
    high = slab % highs
    core = blk % 2
    low = blk // 2
    spot = high * blocks + blk
    rows = coefs // blocks
    wide = 2 * rows
    total = spheres * wide
    waves = gather_ref.shape[0] // 2
    loads = [
        pltpu.make_async_copy(src, dst, load_sem.at[number])
        for number, (src, dst) in enumerate(
            ((plane_hbm, plane_ref), (start_hbm, start_ref), (trans_hbm, trans_ref))
        )
    ]
    for load in loads:
        load.start()

    def far_first(step, size):
        half = (step + 1) // 2
        return lax.rem(size // 2 + jnp.where(lax.rem(step, 2) == 1, -half, half), size)

    ring_x = 4 if quads == 32 else 1
    ring_z = quads // ring_x

    def plane_quad(step):
        place_x = lax.rem(quad // ring_z + far_first(lax.rem(step, ring_x), ring_x), ring_x)
        place_z = lax.rem(lax.rem(quad, ring_z) + far_first(step // ring_x, ring_z), ring_z)
        return place_x * ring_z + place_z

    def plane_peer(step):
        return (plane_quad(step) * highs + high, blk)

    def line_peer(step):
        place = lax.rem(2 * high + low + far_first(step // 2, 2 * highs), 2 * highs)
        side = lax.rem(core + 1 - lax.rem(step, 2), 2)
        return (quad * highs + place // 2, lax.rem(place, 2) * 2 + side)

    barrier = pltpu.get_barrier_semaphore()

    @pl.loop(0, quads - 1)
    def _(step):
        pl.semaphore_signal(barrier, inc=1, device_id=plane_peer(step), device_id_type=MESH)

    @pl.loop(0, line_size - 1)
    def _(step):
        pl.semaphore_signal(barrier, inc=1, device_id=line_peer(step), device_id_type=MESH)

    def chain_peer(step):
        place = lax.rem(2 * slab + low + step + 2 * slabs, 2 * slabs)
        return (place // 2, lax.rem(place, 2) * 2 + core)

    for step in (-1, 1):
        pl.semaphore_signal(barrier, inc=1, device_id=chain_peer(step), device_id_type=MESH)
    greeted = quads - 1 + line_size - 1 + 2

    even = (lax.broadcasted_iota(jnp.int32, (wide, 128), 0) % 2) == 0

    def make_piece(turn, source):
        for sphere in range(spheres):
            for part in range(2):
                stage_ref[0, pl.ds((2 * sphere + part) * rows, rows), :] = source[
                    pl.ds(sphere * wide + part, rows, stride=2), :
                ]
        piece_ref[turn] = stage_ref[0].astype(jnp.bfloat16)

    def send(src, dst, sems, slot, device):
        return pltpu.make_async_remote_copy(
            src_ref=src,
            dst_ref=dst,
            send_sem=send_sem.at[slot],
            recv_sem=sems,
            device_id=device,
            device_id_type=MESH,
        )

    partner = (slab, low * 2 + 1 - core)

    def slot_of(turn, offset, viewer=0):
        place = (low + offset + 4) // 2 - (low + viewer + 4) // 2 + 1
        return turn, place, lax.rem(low + offset + 4, 2) * 2 + core

    def relay(turn, offset, step, number):
        target = slot_of(turn, offset, step)
        src = piece_ref.at[turn] if number < 2 else halo_ref.at[slot_of(turn, offset)]
        return send(
            src, halo_ref.at[target], halo_sem.at[target], 24 + 11 * turn + number, chain_peer(step)
        )

    def share(turn, offset, number):
        slot = slot_of(turn, offset)
        src = piece_ref.at[turn] if number == 5 else halo_ref.at[slot]
        return send(src, halo_ref.at[slot], halo_sem.at[slot], 24 + 11 * turn + number, partner)

    def arrive(turn, offset):
        slot = slot_of(turn, offset)
        ref = halo_ref.at[slot]
        send(ref, ref, halo_sem.at[slot], 24 + 11 * turn, partner).wait_recv()

    toward = 1 - 2 * low

    def halo_copies(turn):
        return (
            [relay(turn, 0, 1, 0), relay(turn, 0, -1, 1), relay(turn, -1, 1, 2)]
            + [relay(turn, 1, -1, 3), relay(turn, -2 * toward, toward, 4), share(turn, 0, 5)]
            + [share(turn, -1, 6), share(turn, 1, 7), share(turn, -2, 8), share(turn, 2, 9)]
            + [share(turn, 3 * toward, 10)]
        )

    def start_halo(turn):
        copies = halo_copies(turn)
        for number in (0, 1, 5):
            copies[number].start()

    def exchange(src_of, dst, turn_slot, peer, size):
        @pl.loop(0, size - 1)
        def _(step):
            send(src_of(step), dst, recv_sem.at[turn_slot], turn_slot, peer(step)).start()

    def drain(block, turn_slot, size, what):
        ref = block.at[pl.ds(0, size - 1)]
        copy = send(ref, ref, recv_sem.at[turn_slot], turn_slot, (slab, blk))
        if what == "recv":
            copy.wait_recv()
        else:
            copy.wait_send()

    def project(field):
        rounded = jnp.concatenate(
            [
                field[sphere * wide : (sphere + 1) * wide].astype(jnp.bfloat16)
                for sphere in range(spheres)
            ],
            axis=1,
        )
        product = jnp.dot(gather_ref[...], rounded, preferred_element_type=jnp.float32)
        sum_re = jnp.zeros((waves, 128), jnp.float32)
        sum_im = jnp.zeros((waves, 128), jnp.float32)
        for sphere in range(spheres):
            lanes = slice(128 * sphere, 128 * (sphere + 1))
            part_re = product[:waves, lanes]
            part_im = product[waves:, lanes]
            cos_part = trig_ref[:, sphere : sphere + 1]
            sin_part = trig_ref[:, spheres + sphere : spheres + sphere + 1]
            sum_re = sum_re + cos_part * part_re + sin_part * part_im
            sum_im = sum_im + cos_part * part_im - sin_part * part_re
        return sum_re, sum_im

    def cut(turn, sums):
        shards = waves // ROWS
        for part in range(2):
            cut_ref[turn, pl.ds(part * shards, shards)] = (
                sums[part].astype(jnp.bfloat16).reshape(shards, ROWS, 128)
            )

    shard_count = 2 * waves // ROWS
    per_device = shard_count // quads

    def shards_of(ref, turn, owner):
        return ref.at[turn, pl.ds(owner * per_device, per_device)]

    def start_scatter(turn):
        exchange(
            lambda step: shards_of(cut_ref, turn, plane_quad(step)),
            part_ref.at[turn, quad],
            10 * turn + 2,
            plane_peer,
            quads,
        )

    def finish_scatter(turn):
        part_ref[turn, quad] = cut_ref[turn, pl.ds(quad * per_device, per_device)]
        drain(part_ref.at[turn], 10 * turn + 2, quads, "recv")
        value = part_ref[turn].astype(jnp.float32).sum(axis=0)
        line_ref[turn, spot] = value.astype(jnp.bfloat16)

    def start_line(turn):
        exchange(
            lambda step: line_ref.at[turn, spot],
            line_ref.at[turn, spot],
            10 * turn + 3,
            line_peer,
            line_size,
        )

    def finish_line(turn):
        drain(line_ref.at[turn], 10 * turn + 3, line_size, "recv")
        value = line_ref[turn].astype(jnp.float32).sum(axis=0)
        sums_ref[turn, pl.ds(quad * per_device, per_device)] = value.astype(jnp.bfloat16)

    def start_gather(turn):
        exchange(
            lambda step: shards_of(sums_ref, turn, quad),
            shards_of(sums_ref, turn, quad),
            10 * turn + 4,
            plane_peer,
            quads,
        )

    def finish_gather(turn):
        ref = sums_ref.at[turn, pl.ds(0, (quads - 1) * per_device)]
        send(ref, ref, recv_sem.at[10 * turn + 4], 10 * turn + 4, (slab, blk)).wait_recv()

    def far_field(turn):
        shards = waves // ROWS
        sum_re = sums_ref[turn, pl.ds(0, shards)].astype(jnp.float32).reshape(waves, 128)
        sum_im = sums_ref[turn, pl.ds(shards, shards)].astype(jnp.float32).reshape(waves, 128)
        weight = trig_ref[:, 2 * spheres : 2 * spheres + 1]
        turned_re, turned_im = [], []
        for sphere in range(spheres):
            cos_part = weight * trig_ref[:, sphere : sphere + 1]
            sin_part = weight * trig_ref[:, spheres + sphere : spheres + sphere + 1]
            turned_re.append((cos_part * sum_re - sin_part * sum_im).astype(jnp.bfloat16))
            turned_im.append((cos_part * sum_im + sin_part * sum_re).astype(jnp.bfloat16))
        turned = jnp.concatenate(
            [jnp.concatenate(turned_re, axis=1), jnp.concatenate(turned_im, axis=1)], axis=0
        )
        return jnp.dot(spread_ref[...], turned, preferred_element_type=jnp.float32)

    def join(turn, place):
        for index in range(blocks):
            stage_ref[index] = halo_ref[turn, place, index].astype(jnp.float32)
        for sphere in range(spheres):
            for part in range(2):
                for index in range(blocks):
                    join_ref[
                        pl.ds(index * rows, rows), pl.ds(128 * part, 128)
                    ] = stage_ref[index, pl.ds((2 * sphere + part) * rows, rows), :]
            joined_ref[place * spheres + sphere] = join_ref[...].astype(jnp.bfloat16)

    def near_field(sphere):
        total_product = jnp.zeros((wide, 256), jnp.float32)
        for pair in range(pairs):
            number = sphere * pairs + pair
            source = (shift_ref[sphere, pair] + 1) * spheres + member_ref[sphere, pair]
            total_product = total_product + jnp.dot(
                trans_ref[number].reshape(wide, coefs),
                joined_ref[source],
                preferred_element_type=jnp.float32,
            )
        swapped = pair_swap(total_product[:, 128:], even)
        near_ref[pl.ds(sphere * wide, wide), :] = total_product[:, :128] + jnp.where(
            even, -swapped, swapped
        )

    def operator(turn, source, sums):
        cut(turn, sums)
        start_scatter(turn)
        copies = halo_copies(turn)
        halo_ref[turn, 1, blk] = piece_ref[turn]
        for offset, numbers in ((-1, (2, 6)), (1, (3, 7))):
            arrive(turn, offset)
            for number in numbers:
                copies[number].start()
        finish_scatter(turn)
        start_line(turn)
        arrive(turn, -2 * toward)
        copies[4].start()
        arrive(turn, 2 * toward)
        for number in (8, 9):
            copies[number].start()
        finish_line(turn)
        start_gather(turn)
        if turn == 1:
            turn_gram(0, 20)
        arrive(turn, 3 * toward)
        copies[10].start()
        for place in (1, 0, 2):
            for side in (0, 1):
                index = side * 2 + 1 - core
                ref = halo_ref.at[turn, place, index]
                send(ref, ref, halo_sem.at[turn, place, index], 24 + 11 * turn, partner).wait_recv()
            join(turn, place)
        if turn == 0:
            loads[2].wait()
        for sphere in range(spheres):
            near_field(sphere)
        if turn == 0:
            spread_mie()
        finish_gather(turn)
        far = far_field(turn)
        out = []
        for sphere in range(spheres):
            span = slice(sphere * wide, (sphere + 1) * wide)
            summed = near_ref[span] + far[:, 128 * sphere : 128 * (sphere + 1)]
            swapped = pair_swap(summed, even)
            out.append(mie_ref[0, span] * summed + mie_ref[1, span] * swapped)
        return out

    def make_trig():
        cos_rows, sin_rows = [], []
        for sphere in range(spheres):
            turns = jnp.zeros((1, waves), jnp.float32)
            for axis in range(3):
                turns = turns + wave_ref[axis : axis + 1, :].astype(jnp.float32) * (
                    position_ref[sphere, axis]
                )
            angle = two_pi * (turns - jnp.round(turns))
            cos_rows.append(jnp.cos(angle))
            sin_rows.append(jnp.sin(angle))
        lines = cos_rows + sin_rows + [weight_ref[...]]
        lines.append(jnp.zeros((128 - len(lines), waves), jnp.float32))
        trig_ref[...] = jnp.concatenate(lines, axis=0).T

    def make_plane():
        upper = jnp.concatenate([plane_ref[0], plane_ref[1]], axis=1)
        lower = jnp.concatenate([-plane_ref[1], plane_ref[0]], axis=1)
        row = lax.broadcasted_iota(jnp.int32, (wide, coefs), 0)
        hit = lax.broadcasted_iota(jnp.int32, (wide, coefs), 1) == blk * rows + row // 2
        real = jnp.where(hit & (row % 2 == 0), 1.0, 0.0).astype(jnp.bfloat16)
        imag = jnp.where(hit & (row % 2 == 1), 1.0, 0.0).astype(jnp.bfloat16)
        own = jnp.dot(real, upper, preferred_element_type=jnp.float32) + jnp.dot(
            imag, lower, preferred_element_type=jnp.float32
        )
        spread_ref[...] = own.astype(jnp.bfloat16)
        gather_ref[...] = own.T.astype(jnp.bfloat16)

    def spread_mie():
        lines = jnp.concatenate(
            [mie_in_ref[sphere] for sphere in range(spheres)]
            + [jnp.zeros((128 - 2 * spheres, rows), jnp.float32)],
            axis=0,
        )
        lines = jnp.concatenate([lines, jnp.zeros((128, 128 - rows), jnp.float32)], axis=1).T
        for sphere in range(spheres):
            real = jnp.broadcast_to(lines[:rows, 2 * sphere : 2 * sphere + 1], (rows, 128))
            imag = jnp.broadcast_to(lines[:rows, 2 * sphere + 1 : 2 * sphere + 2], (rows, 128))
            base = sphere * wide
            mie_ref[0, pl.ds(base, rows, stride=2), :] = real
            mie_ref[0, pl.ds(base + 1, rows, stride=2), :] = real
            mie_ref[1, pl.ds(base, rows, stride=2), :] = -imag
            mie_ref[1, pl.ds(base + 1, rows, stride=2), :] = imag

    make_trig()
    loads[0].wait()
    make_plane()
    loads[1].wait()
    start = [start_ref[sphere * wide : (sphere + 1) * wide] for sphere in range(spheres)]
    make_piece(0, start_ref)
    first_sums = project(start_ref[...])
    pl.semaphore_wait(barrier, greeted)
    start_halo(0)
    image = operator(0, start_ref, first_sums)

    def put_gram(slot, pairs_of):
        lines = []
        for name, left, right in pairs_of:
            real, imag = 0.0, 0.0
            for sphere in range(spheres):
                swapped = pair_swap(right[sphere], even)
                part_re, part_im = inner_rows(left[sphere], right[sphere], swapped, even)
                real, imag = real + part_re, imag + part_im
            lines.append(real)
            if name == "complex":
                lines.append(imag)
        lines.append(jnp.zeros((8 - len(lines), 128), jnp.float32))
        gram_ref[slot, spot] = jnp.concatenate(lines, axis=0)

    def lines_of(slot, place):
        return gram_ref.at[slot, place, pl.ds(0, 4 if slot < 2 else 5)]

    def start_gram(slot, turn_slot):
        exchange(
            lambda step: lines_of(slot, spot),
            lines_of(slot, spot),
            turn_slot,
            line_peer,
            line_size,
        )

    def drain_gram(slot, turn_slot, size, what):
        ref = gram_ref.at[slot, pl.ds(0, size - 1), pl.ds(0, 4 if slot < 2 else 5)]
        copy = send(ref, ref, recv_sem.at[turn_slot], turn_slot, (slab, blk))
        if what == "recv":
            copy.wait_recv()
        else:
            copy.wait_send()

    def turn_gram(slot, turn_slot):
        drain_gram(slot, turn_slot, line_size, "recv")
        gram_ref[slot + 1, quad] = gram_ref[slot, pl.ds(0, line_size)].sum(axis=0)
        exchange(
            lambda step: lines_of(slot + 1, quad),
            lines_of(slot + 1, quad),
            turn_slot + 1,
            plane_peer,
            quads,
        )

    def end_gram(slot, turn_slot):
        drain_gram(slot + 1, turn_slot + 1, quads, "recv")
        return gram_ref[slot + 1, pl.ds(0, quads)].sum(axis=0)

    for sphere in range(spheres):
        image_ref[pl.ds(sphere * wide, wide), :] = image[sphere]
    make_piece(1, image_ref)
    start_halo(1)
    second_sums = project(image_ref[...])
    put_gram(0, (("real", start, start), ("complex", start, image), ("real", image, image)))
    start_gram(0, 20)
    second = operator(1, image_ref, second_sums)
    put_gram(2, (("complex", start, second), ("complex", image, second), ("real", second, second)))
    start_gram(2, 22)
    for sphere in range(spheres):
        second_ref[pl.ds(sphere * wide, wide), :] = second[sphere]
    turn_gram(2, 22)
    early = end_gram(0, 20)
    late = end_gram(2, 22)

    norm_start = early[0:1]
    c_re, c_im = early[1:2], early[2:3]
    norm_image = early[3:4]
    d_re, d_im = late[0:1], late[1:2]
    e_re, e_im = late[2:3], late[3:4]
    norm_second = late[4:5]
    shift = entries * epsilon
    whole = norm_start + shift
    beta = jnp.sqrt(whole / entries)
    h11_re, h11_im = (norm_start - c_re) / whole, -c_im / whole
    g_re, g_im = (shift + c_re) / whole, c_im / whole
    apart = norm_image - (
        2.0 * (g_re * c_re + g_im * c_im) - (g_re * g_re + g_im * g_im) * norm_start
    )
    h21 = jnp.sqrt(jnp.maximum(apart, 0.0) / whole + epsilon)
    scale = 1.0 / (beta * h21)
    a_re, a_im = g_re * scale, g_im * scale
    both = shift / whole * scale / beta
    q_re, q_im = both * (norm_start - c_re), -both * c_im
    over = scale / beta
    gc_re, gc_im = g_re * c_re - g_im * c_im, g_re * c_im + g_im * c_re
    h12_re = (q_re + over * (d_re - gc_re)) / entries
    h12_im = (q_im + over * (d_im - gc_im)) / entries
    u_re = a_re * c_re + a_im * c_im - scale * norm_image
    u_im = a_re * c_im - a_im * c_re
    v_re = a_re * d_re + a_im * d_im - scale * e_re
    v_im = a_re * d_im - a_im * d_re - scale * e_im
    k_re = a_re * u_re - a_im * u_im - scale * v_re + h12_re * q_re + h12_im * q_im
    k_im = a_re * u_im + a_im * u_re - scale * v_im + h12_im * q_re - h12_re * q_im
    kap_re = epsilon / (h21 * h21) + k_re / entries
    kap_im = k_im / entries
    h22_re, h22_im = 1.0 - kap_re, -kap_im
    x_re = a_re * kap_re - a_im * kap_im - h12_re / beta
    x_im = a_re * kap_im + a_im * kap_re - h12_im / beta
    y_re = -scale * kap_re - a_re
    y_im = -scale * kap_im - a_im
    xy_re, xy_im = x_re * y_re + x_im * y_im, x_re * y_im - x_im * y_re
    left = (
        (x_re * x_re + x_im * x_im) * norm_start
        + (y_re * y_re + y_im * y_im) * norm_image
        + scale * scale * norm_second
        + 2.0 * (xy_re * c_re - xy_im * c_im)
        + 2.0 * scale * (x_re * d_re + x_im * d_im)
        + 2.0 * scale * (y_re * e_re + y_im * e_im)
    )
    h32 = jnp.sqrt(jnp.maximum(left, 0.0) / entries + epsilon)
    out_ref[...] = jnp.concatenate(
        [beta, h11_re, h11_im, h21, h12_re, h12_im, h22_re, h22_im, h32]
        + [a_re, a_im, x_re, x_im, y_re, y_im, scale, jnp.zeros((8, 128), jnp.float32)],
        axis=0,
    )

    for turn in range(2):
        for copy in halo_copies(turn):
            copy.wait_send()
        for slot, size, block in (
            (2, quads, part_ref.at[turn]),
            (3, line_size, line_ref.at[turn]),
            (4, quads, part_ref.at[turn]),
        ):
            drain(block, 10 * turn + slot, size, "send")
    for slot in (0, 2):
        drain_gram(slot, 20 + slot, line_size, "send")
        drain_gram(slot + 1, 21 + slot, quads, "send")


def combine_kernel(
    spheres, scalar_ref, start_ref, image_ref, second_ref, next_ref, residual_ref, hess_ref
):
    wide = start_ref.shape[0] // spheres
    even = (lax.broadcasted_iota(jnp.int32, (wide, 128), 0) % 2) == 0
    hess_ref[...] = scalar_ref[0:9, :]
    a_re, a_im, x_re, x_im, y_re, y_im, scale = (
        scalar_ref[9 + number : 10 + number, :] for number in range(7)
    )
    for sphere in range(spheres):
        span = pl.ds(sphere * wide, wide)
        one = start_ref[span, :]
        two = image_ref[span, :]
        one_swapped, two_swapped = pair_swap(one, even), pair_swap(two, even)
        next_ref[span, :] = complex_rows(a_re, a_im, one, one_swapped, even) - scale * two
        residual_ref[span, :] = (
            complex_rows(x_re, x_im, one, one_swapped, even)
            + complex_rows(y_re, y_im, two, two_swapped, even)
            + scale * second_ref[span, :]
        )


def per_device(
    quads,
    highs,
    incident,
    mie_coef,
    translation,
    pair_shift,
    pair_member,
    positions,
    wave_index,
    plane_coef,
    ewald_weight,
):
    spheres, _, rows, fields = incident.shape
    pairs = translation.shape[1]
    coefs = translation.shape[4]
    waves = plane_coef.shape[0]
    total = spheres * 2 * rows
    entries = quads * highs * spheres * coefs
    blocks = coefs // rows
    line_size = highs * blocks
    start = incident.transpose(0, 2, 1, 3).reshape(total, fields)
    trans = translation.transpose(0, 1, 3, 2, 4).reshape(spheres * pairs, rows, 2, coefs)
    shard_count = 2 * waves // ROWS
    per_quad = shard_count // quads
    vmem = pl.BlockSpec(memory_space=pltpu.VMEM)
    smem = pl.BlockSpec(memory_space=pltpu.SMEM)
    hbm = pl.BlockSpec(memory_space=pl.ANY)
    vector = jax.ShapeDtypeStruct((total, fields), jnp.float32)
    kept = pltpu.VMEM((total, fields), jnp.float32)
    first, image, second, scalars = pl.pallas_call(
        functools.partial(kernel, quads, highs, spheres, pairs, coefs, entries),
        out_shape=(kept, kept, kept, pltpu.VMEM((24, fields), jnp.float32)),
        in_specs=[smem, smem, smem, vmem, vmem, vmem, hbm, hbm, hbm],
        out_specs=(vmem, vmem, vmem, vmem),
        scratch_shapes=[
            pltpu.VMEM((2, coefs, waves), jnp.bfloat16),
            pltpu.VMEM((spheres * pairs, rows, 2, coefs), jnp.bfloat16),
            pltpu.VMEM((2 * waves, 2 * rows), jnp.bfloat16),
            pltpu.VMEM((2 * rows, 2 * waves), jnp.bfloat16),
            pltpu.VMEM((waves, 128), jnp.float32),
            pltpu.VMEM((2, total, fields), jnp.float32),
            pltpu.VMEM((2, total, fields), jnp.bfloat16),
            pltpu.VMEM((2, 3, blocks, total, fields), jnp.bfloat16),
            pltpu.VMEM((blocks, total, fields), jnp.float32),
            pltpu.VMEM((coefs, 2 * fields), jnp.float32),
            pltpu.VMEM((3 * spheres, coefs, 2 * fields), jnp.bfloat16),
            pltpu.VMEM((2, shard_count, ROWS, fields), jnp.bfloat16),
            pltpu.VMEM((2, quads, per_quad, ROWS, fields), jnp.bfloat16),
            pltpu.VMEM((2, line_size, per_quad, ROWS, fields), jnp.bfloat16),
            pltpu.VMEM((2, shard_count, ROWS, fields), jnp.bfloat16),
            pltpu.VMEM((4, max(quads, line_size), 8, fields), jnp.float32),
            pltpu.VMEM((total, fields), jnp.float32),
            pltpu.SemaphoreType.DMA((46,)),
            pltpu.SemaphoreType.DMA((24,)),
            pltpu.SemaphoreType.DMA((2, 3, blocks)),
            pltpu.SemaphoreType.DMA((3,)),
        ],
        compiler_params=pltpu.CompilerParams(collective_id=0, has_side_effects=True),
        name="arnoldi",
    )(
        pair_shift,
        pair_member,
        positions,
        wave_index.T,
        ewald_weight.reshape(1, waves),
        mie_coef,
        start,
        plane_coef.transpose(1, 2, 0),
        trans,
    )
    kept_values = (
        pltpu.with_memory_space_constraint(value, pltpu.VMEM)
        for value in (scalars, first, image, second)
    )
    basis, residual, hess = pl.pallas_call(
        functools.partial(combine_kernel, spheres),
        out_shape=(vector, vector, jax.ShapeDtypeStruct((9, fields), jnp.float32)),
        in_specs=[vmem] * 4,
        out_specs=(vmem, vmem, vmem),
        name="combine",
    )(*kept_values)

    def unpacked(field):
        return field.reshape(spheres, rows, 2, fields).transpose(0, 2, 1, 3)

    return unpacked(basis), unpacked(residual), hess


def solution(mesh):
    highs = 4 if mesh.shape[SLAB] % 4 == 0 and mesh.shape[SLAB] > 4 else 2
    quads = mesh.shape[SLAB] // highs
    return jax.shard_map(
        functools.partial(per_device, quads, highs),
        mesh=mesh,
        in_specs=(
            P(SLAB, None, BLK, None),
            P(SLAB, None, BLK),
            P(SLAB, None, None, BLK, None),
            P(SLAB, None),
            P(SLAB, None),
            P(SLAB, None),
            P(),
            P(),
            P(),
        ),
        out_specs=(P(SLAB, None, BLK, None), P(SLAB, None, BLK, None), P()),
        check_vma=False,
    )
```

```python
import functools

import jax
import jax.numpy as jnp
from jax import lax
from jax.experimental import pallas as pl
from jax.experimental.pallas import tpu as pltpu
from jax.sharding import PartitionSpec as P

MESH = pl.DeviceIdType.MESH
SLAB = "slab"
BLK = "blk"
two_pi = 6.283185307179586
epsilon = 1e-06

ROWS = 16


def pair_swap(field, even):
    count = field.shape[0]
    return jnp.where(even, pltpu.roll(field, count - 1, 0), pltpu.roll(field, 1, 0))


def complex_rows(coef_re, coef_im, field, swapped, even):
    return coef_re * field + jnp.where(even, -coef_im, coef_im) * swapped


def inner_rows(left, right, right_swapped, even):
    real = jnp.sum(left * right, axis=0, keepdims=True)
    cross = left * right_swapped
    imag = jnp.sum(jnp.where(even, cross, -cross), axis=0, keepdims=True)
    return real, imag


def kernel(
    quads,
    highs,
    spheres,
    pairs,
    coefs,
    entries,
    shift_hbm,
    member_hbm,
    position_hbm,
    wave_hbm,
    weight_hbm,
    mie_hbm,
    start_hbm,
    plane_hbm,
    trans_hbm,
    start_ref,
    image_ref,
    second_ref,
    out_ref,
    plane_ref,
    trans_ref,
    gather_ref,
    spread_ref,
    trig_ref,
    mie_ref,
    piece_ref,
    halo_ref,
    stage_ref,
    join_ref,
    joined_ref,
    cut_ref,
    part_ref,
    line_ref,
    sums_ref,
    gram_ref,
    near_ref,
    send_sem,
    recv_sem,
    halo_sem,
    load_sem,
    shift_ref,
    member_ref,
    position_ref,
    wave_ref,
    weight_ref,
    mie_in_ref,
):
    blocks = 4
    slabs = quads * highs
    line_size = highs * blocks
    slab = lax.axis_index(SLAB)
    blk = lax.axis_index(BLK)
    quad = slab // highs
    high = slab % highs
    core = blk % 2
    low = blk // 2
    spot = high * blocks + blk
    rows = coefs // blocks
    wide = 2 * rows
    total = spheres * wide
    waves = gather_ref.shape[0] // 2
    loads = [
        pltpu.make_async_copy(src, dst, load_sem.at[number])
        for number, (src, dst) in enumerate(
            (
                (plane_hbm, plane_ref),
                (start_hbm, start_ref),
                (trans_hbm, trans_ref),
                (position_hbm, position_ref),
                (wave_hbm, wave_ref),
                (weight_hbm, weight_ref),
                (shift_hbm, shift_ref),
                (member_hbm, member_ref),
                (mie_hbm, mie_in_ref),
            )
        )
    ]

    def far_first(step, size):
        half = (step + 1) // 2
        return lax.rem(size // 2 + jnp.where(lax.rem(step, 2) == 1, -half, half), size)

    ring_x = 4 if quads == 32 else 1
    ring_z = quads // ring_x

    def plane_quad(step):
        place_x = lax.rem(quad // ring_z + far_first(lax.rem(step, ring_x), ring_x), ring_x)
        place_z = lax.rem(lax.rem(quad, ring_z) + far_first(step // ring_x, ring_z), ring_z)
        return place_x * ring_z + place_z

    def plane_peer(step):
        return (plane_quad(step) * highs + high, blk)

    def line_peer(step):
        place = lax.rem(2 * high + low + far_first(step // 2, 2 * highs), 2 * highs)
        side = lax.rem(core + 1 - lax.rem(step, 2), 2)
        return (quad * highs + place // 2, lax.rem(place, 2) * 2 + side)

    barrier = pltpu.get_barrier_semaphore()

    @pl.loop(0, quads - 1)
    def _(step):
        pl.semaphore_signal(barrier, inc=1, device_id=plane_peer(step), device_id_type=MESH)

    @pl.loop(0, line_size - 1)
    def _(step):
        pl.semaphore_signal(barrier, inc=1, device_id=line_peer(step), device_id_type=MESH)

    def chain_peer(step):
        place = lax.rem(2 * slab + low + step + 2 * slabs, 2 * slabs)
        return (place // 2, lax.rem(place, 2) * 2 + core)

    for step in (-1, 1):
        pl.semaphore_signal(barrier, inc=1, device_id=chain_peer(step), device_id_type=MESH)
    greeted = quads - 1 + line_size - 1 + 2

    for number in (3, 4, 5, 0, 1, 6, 7, 8, 2):
        loads[number].start()

    even = (lax.broadcasted_iota(jnp.int32, (wide, 128), 0) % 2) == 0

    def make_piece(turn, source):
        for sphere in range(spheres):
            for part in range(2):
                stage_ref[0, pl.ds((2 * sphere + part) * rows, rows), :] = source[
                    pl.ds(sphere * wide + part, rows, stride=2), :
                ]
        piece_ref[turn] = stage_ref[0].astype(jnp.bfloat16)

    def send(src, dst, sems, slot, device):
        return pltpu.make_async_remote_copy(
            src_ref=src,
            dst_ref=dst,
            send_sem=send_sem.at[slot],
            recv_sem=sems,
            device_id=device,
            device_id_type=MESH,
        )

    partner = (slab, low * 2 + 1 - core)

    def slot_of(turn, offset, viewer=0):
        place = (low + offset + 4) // 2 - (low + viewer + 4) // 2 + 1
        return turn, place, lax.rem(low + offset + 4, 2) * 2 + core

    def relay(turn, offset, step, number):
        target = slot_of(turn, offset, step)
        src = piece_ref.at[turn] if number < 2 else halo_ref.at[slot_of(turn, offset)]
        return send(
            src, halo_ref.at[target], halo_sem.at[target], 24 + 11 * turn + number, chain_peer(step)
        )

    def share(turn, offset, number):
        slot = slot_of(turn, offset)
        src = piece_ref.at[turn] if number == 5 else halo_ref.at[slot]
        return send(src, halo_ref.at[slot], halo_sem.at[slot], 24 + 11 * turn + number, partner)

    def arrive(turn, offset):
        slot = slot_of(turn, offset)
        ref = halo_ref.at[slot]
        send(ref, ref, halo_sem.at[slot], 24 + 11 * turn, partner).wait_recv()

    toward = 1 - 2 * low

    def halo_copies(turn):
        return (
            [relay(turn, 0, 1, 0), relay(turn, 0, -1, 1), relay(turn, -1, 1, 2)]
            + [relay(turn, 1, -1, 3), relay(turn, -2 * toward, toward, 4), share(turn, 0, 5)]
            + [share(turn, -1, 6), share(turn, 1, 7), share(turn, -2, 8), share(turn, 2, 9)]
            + [share(turn, 3 * toward, 10)]
        )

    def start_halo(turn):
        copies = halo_copies(turn)
        for number in (0, 1, 5):
            copies[number].start()

    def exchange(src_of, dst, turn_slot, peer, size):
        @pl.loop(0, size - 1)
        def _(step):
            send(src_of(step), dst, recv_sem.at[turn_slot], turn_slot, peer(step)).start()

    def drain(block, turn_slot, size, what):
        ref = block.at[pl.ds(0, size - 1)]
        copy = send(ref, ref, recv_sem.at[turn_slot], turn_slot, (slab, blk))
        if what == "recv":
            copy.wait_recv()
        else:
            copy.wait_send()

    def project(field):
        rounded = jnp.concatenate(
            [
                field[sphere * wide : (sphere + 1) * wide].astype(jnp.bfloat16)
                for sphere in range(spheres)
            ],
            axis=1,
        )
        product = jnp.dot(gather_ref[...], rounded, preferred_element_type=jnp.float32)
        sum_re = jnp.zeros((waves, 128), jnp.float32)
        sum_im = jnp.zeros((waves, 128), jnp.float32)
        for sphere in range(spheres):
            lanes = slice(128 * sphere, 128 * (sphere + 1))
            part_re = product[:waves, lanes]
            part_im = product[waves:, lanes]
            cos_part = trig_ref[:, sphere : sphere + 1]
            sin_part = trig_ref[:, spheres + sphere : spheres + sphere + 1]
            sum_re = sum_re + cos_part * part_re + sin_part * part_im
            sum_im = sum_im + cos_part * part_im - sin_part * part_re
        return sum_re, sum_im

    def cut(turn, sums):
        shards = waves // ROWS
        for part in range(2):
            cut_ref[turn, pl.ds(part * shards, shards)] = (
                sums[part].astype(jnp.bfloat16).reshape(shards, ROWS, 128)
            )

    shard_count = 2 * waves // ROWS
    per_device = shard_count // quads

    def shards_of(ref, turn, owner):
        return ref.at[turn, pl.ds(owner * per_device, per_device)]

    def start_scatter(turn):
        exchange(
            lambda step: shards_of(cut_ref, turn, plane_quad(step)),
            part_ref.at[turn, quad],
            10 * turn + 2,
            plane_peer,
            quads,
        )

    def finish_scatter(turn):
        part_ref[turn, quad] = cut_ref[turn, pl.ds(quad * per_device, per_device)]
        drain(part_ref.at[turn], 10 * turn + 2, quads, "recv")
        value = part_ref[turn].astype(jnp.float32).sum(axis=0)
        line_ref[turn, spot] = value.astype(jnp.bfloat16)

    def start_line(turn):
        exchange(
            lambda step: line_ref.at[turn, spot],
            line_ref.at[turn, spot],
            10 * turn + 3,
            line_peer,
            line_size,
        )

    def finish_line(turn):
        drain(line_ref.at[turn], 10 * turn + 3, line_size, "recv")
        value = line_ref[turn].astype(jnp.float32).sum(axis=0)
        sums_ref[turn, pl.ds(quad * per_device, per_device)] = value.astype(jnp.bfloat16)

    def start_gather(turn):
        exchange(
            lambda step: shards_of(sums_ref, turn, quad),
            shards_of(sums_ref, turn, quad),
            10 * turn + 4,
            plane_peer,
            quads,
        )

    def finish_gather(turn):
        ref = sums_ref.at[turn, pl.ds(0, (quads - 1) * per_device)]
        send(ref, ref, recv_sem.at[10 * turn + 4], 10 * turn + 4, (slab, blk)).wait_recv()

    def far_field(turn):
        shards = waves // ROWS
        sum_re = sums_ref[turn, pl.ds(0, shards)].astype(jnp.float32).reshape(waves, 128)
        sum_im = sums_ref[turn, pl.ds(shards, shards)].astype(jnp.float32).reshape(waves, 128)
        weight = trig_ref[:, 2 * spheres : 2 * spheres + 1]
        turned_re, turned_im = [], []
        for sphere in range(spheres):
            cos_part = weight * trig_ref[:, sphere : sphere + 1]
            sin_part = weight * trig_ref[:, spheres + sphere : spheres + sphere + 1]
            turned_re.append((cos_part * sum_re - sin_part * sum_im).astype(jnp.bfloat16))
            turned_im.append((cos_part * sum_im + sin_part * sum_re).astype(jnp.bfloat16))
        turned = jnp.concatenate(
            [jnp.concatenate(turned_re, axis=1), jnp.concatenate(turned_im, axis=1)], axis=0
        )
        return jnp.dot(spread_ref[...], turned, preferred_element_type=jnp.float32)

    def join(turn, place):
        for index in range(blocks):
            stage_ref[index] = halo_ref[turn, place, index].astype(jnp.float32)
        for sphere in range(spheres):
            for part in range(2):
                for index in range(blocks):
                    join_ref[
                        pl.ds(index * rows, rows), pl.ds(128 * part, 128)
                    ] = stage_ref[index, pl.ds((2 * sphere + part) * rows, rows), :]
            joined_ref[place * spheres + sphere] = join_ref[...].astype(jnp.bfloat16)

    def near_field(sphere):
        total_product = jnp.zeros((wide, 256), jnp.float32)
        for pair in range(pairs):
            number = sphere * pairs + pair
            source = (shift_ref[sphere, pair] + 1) * spheres + member_ref[sphere, pair]
            total_product = total_product + jnp.dot(
                trans_ref[number].reshape(wide, coefs),
                joined_ref[source],
                preferred_element_type=jnp.float32,
            )
        swapped = pair_swap(total_product[:, 128:], even)
        near_ref[pl.ds(sphere * wide, wide), :] = total_product[:, :128] + jnp.where(
            even, -swapped, swapped
        )

    def operator(turn, source, sums):
        if turn == 1:
            cut(turn, sums)
        start_scatter(turn)
        copies = halo_copies(turn)
        if turn == 1:
            put_gram(
                0,
                (
                    ("real", start, start),
                    ("complex", start, image),
                    ("real", image, image),
                ),
            )
            start_gram(0, 20)
        halo_ref[turn, 1, blk] = piece_ref[turn]
        for offset, numbers in ((-1, (2, 6)), (1, (3, 7))):
            arrive(turn, offset)
            for number in numbers:
                copies[number].start()
        finish_scatter(turn)
        start_line(turn)
        arrive(turn, -2 * toward)
        copies[4].start()
        arrive(turn, 2 * toward)
        for number in (8, 9):
            copies[number].start()
        finish_line(turn)
        start_gather(turn)
        if turn == 1:
            turn_gram(0, 20)
        arrive(turn, 3 * toward)
        copies[10].start()
        for place in (1, 0, 2):
            for side in (0, 1):
                index = side * 2 + 1 - core
                ref = halo_ref.at[turn, place, index]
                send(ref, ref, halo_sem.at[turn, place, index], 24 + 11 * turn, partner).wait_recv()
            join(turn, place)
        if turn == 0:
            for number in (2, 6, 7, 8):
                loads[number].wait()
        for sphere in range(spheres):
            near_field(sphere)
        if turn == 0:
            spread_mie()
        finish_gather(turn)
        far = far_field(turn)
        out = []
        for sphere in range(spheres):
            span = slice(sphere * wide, (sphere + 1) * wide)
            summed = near_ref[span] + far[:, 128 * sphere : 128 * (sphere + 1)]
            swapped = pair_swap(summed, even)
            out.append(mie_ref[0, span] * summed + mie_ref[1, span] * swapped)
        return out

    def make_trig():
        cos_rows, sin_rows = [], []
        for sphere in range(spheres):
            turns = jnp.zeros((1, waves), jnp.float32)
            for axis in range(3):
                turns = turns + wave_ref[axis : axis + 1, :].astype(jnp.float32) * (
                    position_ref[sphere, axis]
                )
            angle = two_pi * (turns - jnp.round(turns))
            cos_rows.append(jnp.cos(angle))
            sin_rows.append(jnp.sin(angle))
        lines = cos_rows + sin_rows + [weight_ref[...]]
        lines.append(jnp.zeros((128 - len(lines), waves), jnp.float32))
        trig_ref[...] = jnp.concatenate(lines, axis=0).T

    def make_plane():
        upper = jnp.concatenate([plane_ref[0], plane_ref[1]], axis=1)
        lower = jnp.concatenate([-plane_ref[1], plane_ref[0]], axis=1)
        row = lax.broadcasted_iota(jnp.int32, (wide, coefs), 0)
        hit = lax.broadcasted_iota(jnp.int32, (wide, coefs), 1) == blk * rows + row // 2
        real = jnp.where(hit & (row % 2 == 0), 1.0, 0.0).astype(jnp.bfloat16)
        imag = jnp.where(hit & (row % 2 == 1), 1.0, 0.0).astype(jnp.bfloat16)
        own = jnp.dot(real, upper, preferred_element_type=jnp.float32) + jnp.dot(
            imag, lower, preferred_element_type=jnp.float32
        )
        spread_ref[...] = own.astype(jnp.bfloat16)
        gather_ref[...] = own.T.astype(jnp.bfloat16)

    def spread_mie():
        lines = jnp.concatenate(
            [mie_in_ref[sphere] for sphere in range(spheres)]
            + [jnp.zeros((128 - 2 * spheres, rows), jnp.float32)],
            axis=0,
        )
        lines = jnp.concatenate([lines, jnp.zeros((128, 128 - rows), jnp.float32)], axis=1).T
        for sphere in range(spheres):
            real = jnp.broadcast_to(lines[:rows, 2 * sphere : 2 * sphere + 1], (rows, 128))
            imag = jnp.broadcast_to(lines[:rows, 2 * sphere + 1 : 2 * sphere + 2], (rows, 128))
            base = sphere * wide
            mie_ref[0, pl.ds(base, rows, stride=2), :] = real
            mie_ref[0, pl.ds(base + 1, rows, stride=2), :] = real
            mie_ref[1, pl.ds(base, rows, stride=2), :] = -imag
            mie_ref[1, pl.ds(base + 1, rows, stride=2), :] = imag

    for number in (3, 4, 5):
        loads[number].wait()
    make_trig()
    loads[0].wait()
    make_plane()
    loads[1].wait()
    start = [start_ref[sphere * wide : (sphere + 1) * wide] for sphere in range(spheres)]
    make_piece(0, start_ref)
    first_sums = project(start_ref[...])
    cut(0, first_sums)
    pl.semaphore_wait(barrier, greeted)
    start_halo(0)
    image = operator(0, start_ref, first_sums)

    def put_gram(slot, pairs_of):
        lines = []
        for name, left, right in pairs_of:
            real, imag = 0.0, 0.0
            for sphere in range(spheres):
                swapped = pair_swap(right[sphere], even)
                part_re, part_im = inner_rows(left[sphere], right[sphere], swapped, even)
                real, imag = real + part_re, imag + part_im
            lines.append(real)
            if name == "complex":
                lines.append(imag)
        lines.append(jnp.zeros((8 - len(lines), 128), jnp.float32))
        gram_ref[slot, spot] = jnp.concatenate(lines, axis=0)

    def lines_of(slot, place):
        return gram_ref.at[slot, place, pl.ds(0, 4 if slot < 2 else 5)]

    def start_gram(slot, turn_slot):
        exchange(
            lambda step: lines_of(slot, spot),
            lines_of(slot, spot),
            turn_slot,
            line_peer,
            line_size,
        )

    def drain_gram(slot, turn_slot, size, what):
        ref = gram_ref.at[slot, pl.ds(0, size - 1), pl.ds(0, 4 if slot < 2 else 5)]
        copy = send(ref, ref, recv_sem.at[turn_slot], turn_slot, (slab, blk))
        if what == "recv":
            copy.wait_recv()
        else:
            copy.wait_send()

    def turn_gram(slot, turn_slot):
        drain_gram(slot, turn_slot, line_size, "recv")
        gram_ref[slot + 1, quad] = gram_ref[slot, pl.ds(0, line_size)].sum(axis=0)
        exchange(
            lambda step: lines_of(slot + 1, quad),
            lines_of(slot + 1, quad),
            turn_slot + 1,
            plane_peer,
            quads,
        )

    def end_gram(slot, turn_slot):
        drain_gram(slot + 1, turn_slot + 1, quads, "recv")
        return gram_ref[slot + 1, pl.ds(0, quads)].sum(axis=0)

    for sphere in range(spheres):
        image_ref[pl.ds(sphere * wide, wide), :] = image[sphere]
    make_piece(1, image_ref)
    start_halo(1)
    second_sums = project(image_ref[...])
    second = operator(1, image_ref, second_sums)
    put_gram(2, (("complex", start, second), ("complex", image, second), ("real", second, second)))
    start_gram(2, 22)
    for sphere in range(spheres):
        second_ref[pl.ds(sphere * wide, wide), :] = second[sphere]
    turn_gram(2, 22)
    early = end_gram(0, 20)
    late = end_gram(2, 22)

    norm_start = early[0:1]
    c_re, c_im = early[1:2], early[2:3]
    norm_image = early[3:4]
    d_re, d_im = late[0:1], late[1:2]
    e_re, e_im = late[2:3], late[3:4]
    norm_second = late[4:5]
    shift = entries * epsilon
    whole = norm_start + shift
    beta = jnp.sqrt(whole / entries)
    h11_re, h11_im = (norm_start - c_re) / whole, -c_im / whole
    g_re, g_im = (shift + c_re) / whole, c_im / whole
    apart = norm_image - (
        2.0 * (g_re * c_re + g_im * c_im) - (g_re * g_re + g_im * g_im) * norm_start
    )
    h21 = jnp.sqrt(jnp.maximum(apart, 0.0) / whole + epsilon)
    scale = 1.0 / (beta * h21)
    a_re, a_im = g_re * scale, g_im * scale
    both = shift / whole * scale / beta
    q_re, q_im = both * (norm_start - c_re), -both * c_im
    over = scale / beta
    gc_re, gc_im = g_re * c_re - g_im * c_im, g_re * c_im + g_im * c_re
    h12_re = (q_re + over * (d_re - gc_re)) / entries
    h12_im = (q_im + over * (d_im - gc_im)) / entries
    u_re = a_re * c_re + a_im * c_im - scale * norm_image
    u_im = a_re * c_im - a_im * c_re
    v_re = a_re * d_re + a_im * d_im - scale * e_re
    v_im = a_re * d_im - a_im * d_re - scale * e_im
    k_re = a_re * u_re - a_im * u_im - scale * v_re + h12_re * q_re + h12_im * q_im
    k_im = a_re * u_im + a_im * u_re - scale * v_im + h12_im * q_re - h12_re * q_im
    kap_re = epsilon / (h21 * h21) + k_re / entries
    kap_im = k_im / entries
    h22_re, h22_im = 1.0 - kap_re, -kap_im
    x_re = a_re * kap_re - a_im * kap_im - h12_re / beta
    x_im = a_re * kap_im + a_im * kap_re - h12_im / beta
    y_re = -scale * kap_re - a_re
    y_im = -scale * kap_im - a_im
    xy_re, xy_im = x_re * y_re + x_im * y_im, x_re * y_im - x_im * y_re
    left = (
        (x_re * x_re + x_im * x_im) * norm_start
        + (y_re * y_re + y_im * y_im) * norm_image
        + scale * scale * norm_second
        + 2.0 * (xy_re * c_re - xy_im * c_im)
        + 2.0 * scale * (x_re * d_re + x_im * d_im)
        + 2.0 * scale * (y_re * e_re + y_im * e_im)
    )
    h32 = jnp.sqrt(jnp.maximum(left, 0.0) / entries + epsilon)
    out_ref[...] = jnp.concatenate(
        [beta, h11_re, h11_im, h21, h12_re, h12_im, h22_re, h22_im, h32]
        + [a_re, a_im, x_re, x_im, y_re, y_im, scale, jnp.zeros((8, 128), jnp.float32)],
        axis=0,
    )

    for turn in range(2):
        for copy in halo_copies(turn):
            copy.wait_send()
        for slot, size, block in (
            (2, quads, part_ref.at[turn]),
            (3, line_size, line_ref.at[turn]),
            (4, quads, part_ref.at[turn]),
        ):
            drain(block, 10 * turn + slot, size, "send")
    for slot in (0, 2):
        drain_gram(slot, 20 + slot, line_size, "send")
        drain_gram(slot + 1, 21 + slot, quads, "send")


def combine_kernel(
    spheres, scalar_ref, start_ref, image_ref, second_ref, next_ref, residual_ref, hess_ref
):
    wide = start_ref.shape[0] // spheres
    even = (lax.broadcasted_iota(jnp.int32, (wide, 128), 0) % 2) == 0
    hess_ref[...] = scalar_ref[0:9, :]
    a_re, a_im, x_re, x_im, y_re, y_im, scale = (
        scalar_ref[9 + number : 10 + number, :] for number in range(7)
    )
    for sphere in range(spheres):
        span = pl.ds(sphere * wide, wide)
        one = start_ref[span, :]
        two = image_ref[span, :]
        one_swapped, two_swapped = pair_swap(one, even), pair_swap(two, even)
        next_ref[span, :] = complex_rows(a_re, a_im, one, one_swapped, even) - scale * two
        residual_ref[span, :] = (
            complex_rows(x_re, x_im, one, one_swapped, even)
            + complex_rows(y_re, y_im, two, two_swapped, even)
            + scale * second_ref[span, :]
        )


def per_device(
    quads,
    highs,
    incident,
    mie_coef,
    translation,
    pair_shift,
    pair_member,
    positions,
    wave_index,
    plane_coef,
    ewald_weight,
):
    spheres, _, rows, fields = incident.shape
    pairs = translation.shape[1]
    coefs = translation.shape[4]
    waves = plane_coef.shape[0]
    total = spheres * 2 * rows
    entries = quads * highs * spheres * coefs
    blocks = coefs // rows
    line_size = highs * blocks
    start = incident.transpose(0, 2, 1, 3).reshape(total, fields)
    trans = translation.transpose(0, 1, 3, 2, 4).reshape(spheres * pairs, rows, 2, coefs)
    shard_count = 2 * waves // ROWS
    per_quad = shard_count // quads
    vmem = pl.BlockSpec(memory_space=pltpu.VMEM)
    hbm = pl.BlockSpec(memory_space=pl.ANY)
    vector = jax.ShapeDtypeStruct((total, fields), jnp.float32)
    kept = pltpu.VMEM((total, fields), jnp.float32)
    first, image, second, scalars = pl.pallas_call(
        functools.partial(kernel, quads, highs, spheres, pairs, coefs, entries),
        out_shape=(kept, kept, kept, pltpu.VMEM((24, fields), jnp.float32)),
        in_specs=[hbm] * 9,
        out_specs=(vmem, vmem, vmem, vmem),
        scratch_shapes=[
            pltpu.VMEM((2, coefs, waves), jnp.bfloat16),
            pltpu.VMEM((spheres * pairs, rows, 2, coefs), jnp.bfloat16),
            pltpu.VMEM((2 * waves, 2 * rows), jnp.bfloat16),
            pltpu.VMEM((2 * rows, 2 * waves), jnp.bfloat16),
            pltpu.VMEM((waves, 128), jnp.float32),
            pltpu.VMEM((2, total, fields), jnp.float32),
            pltpu.VMEM((2, total, fields), jnp.bfloat16),
            pltpu.VMEM((2, 3, blocks, total, fields), jnp.bfloat16),
            pltpu.VMEM((blocks, total, fields), jnp.float32),
            pltpu.VMEM((coefs, 2 * fields), jnp.float32),
            pltpu.VMEM((3 * spheres, coefs, 2 * fields), jnp.bfloat16),
            pltpu.VMEM((2, shard_count, ROWS, fields), jnp.bfloat16),
            pltpu.VMEM((2, quads, per_quad, ROWS, fields), jnp.bfloat16),
            pltpu.VMEM((2, line_size, per_quad, ROWS, fields), jnp.bfloat16),
            pltpu.VMEM((2, shard_count, ROWS, fields), jnp.bfloat16),
            pltpu.VMEM((4, max(quads, line_size), 8, fields), jnp.float32),
            pltpu.VMEM((total, fields), jnp.float32),
            pltpu.SemaphoreType.DMA((46,)),
            pltpu.SemaphoreType.DMA((24,)),
            pltpu.SemaphoreType.DMA((2, 3, blocks)),
            pltpu.SemaphoreType.DMA((9,)),
            pltpu.SMEM(pair_shift.shape, jnp.int32),
            pltpu.SMEM(pair_member.shape, jnp.int32),
            pltpu.SMEM(positions.shape, jnp.float32),
            pltpu.VMEM((3, waves), jnp.int32),
            pltpu.VMEM((1, waves), jnp.float32),
            pltpu.VMEM(mie_coef.shape, jnp.float32),
        ],
        compiler_params=pltpu.CompilerParams(collective_id=0, has_side_effects=True),
        name="arnoldi",
    )(
        pair_shift,
        pair_member,
        positions,
        wave_index.T,
        ewald_weight.reshape(1, waves),
        mie_coef,
        start,
        plane_coef.transpose(1, 2, 0),
        trans,
    )
    kept_values = (
        pltpu.with_memory_space_constraint(value, pltpu.VMEM)
        for value in (scalars, first, image, second)
    )
    basis, residual, hess = pl.pallas_call(
        functools.partial(combine_kernel, spheres),
        out_shape=(vector, vector, jax.ShapeDtypeStruct((9, fields), jnp.float32)),
        in_specs=[vmem] * 4,
        out_specs=(vmem, vmem, vmem),
        name="combine",
    )(*kept_values)

    def unpacked(field):
        return field.reshape(spheres, rows, 2, fields).transpose(0, 2, 1, 3)

    return unpacked(basis), unpacked(residual), hess


def solution(mesh):
    highs = 4 if mesh.shape[SLAB] % 4 == 0 and mesh.shape[SLAB] > 4 else 2
    quads = mesh.shape[SLAB] // highs
    return jax.shard_map(
        functools.partial(per_device, quads, highs),
        mesh=mesh,
        in_specs=(
            P(SLAB, None, BLK, None),
            P(SLAB, None, BLK),
            P(SLAB, None, None, BLK, None),
            P(SLAB, None),
            P(SLAB, None),
            P(SLAB, None),
            P(),
            P(),
            P(),
        ),
        out_specs=(P(SLAB, None, BLK, None), P(SLAB, None, BLK, None), P()),
        check_vma=False,
    )
```
